256 devices in a mesh: member: 2 (over z), band: 128 (over x, y, core).
Axes of the slice: x: 8, y: 8, z: 2, core: 2. Of those that a mesh axis runs over, the one named last changes fastest.
The devices are a block of a 8x8x16 slice.
Arguments:
- grid_in: bfloat16 [256, 274, 5248], P(('member', 'band')), parts along dimension 0, may hold values from -6 to 6
- legendre: bfloat16 [128, 2, 640, 64], P('band'), may hold values from -0.75 to 0.75
- gauss_weight: float32 [64], replicated, may hold values from 0.2 to 2
- vertical_modes: float32 [137, 137], replicated
- coupling: float32 [137, 137], replicated, may hold values from -0.5 to 0.5
- mode_rates: float32 [137], replicated, may hold values from 0.1 to 10
- loop_length: int32 [128], replicated, may hold values from 20 to 5136, as said below
- lat_order: int32 [128], replicated, may hold values from 0 to 127, each once
- wave_number: int32 [128], replicated, may hold values from 0 to 1279, as said below
Outputs:
- grid_out: bfloat16 [256, 274, 5248], P(('member', 'band')), parts along dimension 0
The draws below stay inside these ranges and needn't reach their ends.
There are 2 independent parts, one for each index of `member`. The reference program is written for one: setup_inputs(seed, part) draws one part's arguments, and reference() takes and returns one part's arrays. A program takes and returns all parts, laid end to end along the dimension named above; an argument that names none is the same for every part. Nothing has to cross between parts.
Inputs may be any that keep to these rules, and one draw needn't show every extreme that they name: loop_length[t] = 20 + 4 k with k not falling from the poles toward the equator, equal for latitudes t and 127 - t; the equatorial loops have 5248 - 112 points. Row i of grid_in and grid_out holds latitude lat_order[i]. `wave_number`: distinct values.
All inputs are finite; a program needn't handle non-finite values.
Results may differ from the reference program's by a relative error of at most 0.013.
Values may be sent and summed in bfloat16 or wider, within the bound.
A program may use at most 64 MiB of HBM per device.

```python
import math
import jax
import jax.numpy as jnp
from jax import lax

TRUNC = 1279
LOOP_PAD = 5248
LEV = 137
NLAT = 128
NLAT_H = 64
M_WIN = 128
FL = 274
NHALF = 640


def draw_vertical_modes(key, part):
    gaussian = jax.random.normal(key, (LEV, LEV), jnp.float32)
    basis, upper_part = jnp.linalg.qr(gaussian)
    return basis.astype(jnp.float32)


def draw_loop_length(key, part):
    top_index = (LOOP_PAD - 132) // 4
    loop_key = jax.random.fold_in(key, 7)
    picked = jax.random.randint(loop_key, (NLAT_H,), 0, top_index + 1, dtype=jnp.int32)
    loop_index = jnp.sort(picked)
    loop_index = loop_index.at[NLAT_H - 1].set(top_index)
    north_len = 20 + 4 * loop_index
    return jnp.concatenate([north_len, north_len[::-1]]).astype(jnp.int32)


def draw_wave_number(key, part):
    first_key = jax.random.fold_in(key, 11)
    second_key = jax.random.fold_in(key, 23)
    chosen = jax.random.permutation(first_key, TRUNC + 1)[:M_WIN].astype(jnp.int32)
    has_top = jnp.any(chosen == TRUNC)
    chosen = chosen.at[0].set(jnp.where(has_top, chosen[0], TRUNC))
    has_zero = jnp.any(chosen == 0)
    place = jnp.where(chosen[1] == TRUNC, 2, 1)
    chosen = chosen.at[place].set(jnp.where(has_zero, chosen[place], 0))
    shuffle = jax.random.permutation(second_key, M_WIN)
    return chosen[shuffle].astype(jnp.int32)


def steps_of(stream_key, extent, pieces, smallest, high):
    def one(axis_at, blocks):
        heights = jax.random.uniform(jax.random.fold_in(jax.random.fold_in(stream_key, 6), axis_at), (blocks,), jnp.float32, smallest / len(pieces), high / len(pieces))
        return jnp.repeat(jnp.exp(heights), extent[axis_at] // blocks).reshape((-1,) + (1,) * (len(extent) - axis_at - 1))

    level = one(*pieces[0])
    for cut in pieces[1:]:
        level = level * one(*cut)
    return level


def noise(stream_key, dims, width, reach, cuts=(), kind=jnp.bfloat16):
    gain = steps_of(stream_key, dims, cuts, -0.22, 0.18) if cuts else 1.0
    entries = jax.random.normal(stream_key, dims, jnp.float32) * width * gain
    return jnp.minimum(jnp.maximum(entries, -reach), reach).astype(kind)


def setup_inputs(seed: int = 0, part: int = 0) -> dict:
    key_of = jax.random.split(jax.random.key(seed), 10)
    part_splits = jax.random.split(jax.random.fold_in(key_of[9], part), 10)
    grid_in = noise(part_splits[0], (NLAT, FL, LOOP_PAD), 1.0, 6.0, ((0, 128),))
    legendre = noise(key_of[1], (M_WIN, 2, NHALF, NLAT_H), NLAT_H ** -0.5, 0.75, ((0, 128),))
    gauss_weight = jnp.clip(jnp.exp(jax.random.uniform(key_of[2], (NLAT_H,), jnp.float32, math.log(0.2), math.log(2.0))), 0.2, 2.0)
    vertical_modes = draw_vertical_modes(jax.random.fold_in(key_of[9], 71), part)
    coupling = noise(key_of[4], (LEV, LEV), LEV ** -0.5, 0.5, (), jnp.float32)
    mode_rates = jnp.clip(jnp.exp(jax.random.uniform(key_of[5], (LEV,), jnp.float32, math.log(0.1), math.log(10.0))), 0.1, 10.0)
    loop_length = draw_loop_length(jax.random.fold_in(key_of[9], 71), part)
    lat_order = jax.random.permutation(key_of[7], NLAT).astype(jnp.int32)
    wave_number = draw_wave_number(jax.random.fold_in(key_of[9], 71), part)
    return {"grid_in": grid_in, "legendre": legendre, "gauss_weight": gauss_weight, "vertical_modes": vertical_modes, "coupling": coupling, "mode_rates": mode_rates, "loop_length": loop_length, "lat_order": lat_order, "wave_number": wave_number}


implicit_step = 0.5
highest = lax.Precision.HIGHEST

def loop_tables(length, wave_list, block_count):
    offsets = jnp.arange(128, dtype=jnp.int32)
    inner_turn = offsets[:, None] * wave_list[None, :] % length
    angles = inner_turn.astype(jnp.float32) * (2.0 * math.pi) / length.astype(jnp.float32)
    inner_table = jnp.concatenate([jnp.cos(angles), jnp.sin(angles)], axis=1).astype(jnp.bfloat16)
    block_index = jnp.arange(block_count, dtype=jnp.int32)
    outer_turn = block_index[:, None] * 128 * wave_list[None, :] % length
    phases = outer_turn.astype(jnp.float32) * (2.0 * math.pi) / length.astype(jnp.float32)
    return (inner_table, jnp.cos(phases), jnp.sin(phases))

def forward_loop(one_loop, length, wave_list):
    field_count, loop_width = one_loop.shape
    block_count = loop_width // 128
    wave_count = wave_list.shape[0]
    inner_table, cos_turn, sin_turn = loop_tables(length, wave_list, block_count)
    inside = jnp.arange(loop_width, dtype=jnp.int32) < length
    masked = jnp.where(inside[None, :], one_loop, jnp.zeros((), one_loop.dtype))
    products = jnp.dot(masked.reshape(field_count * block_count, 128).astype(jnp.float32), inner_table.astype(jnp.float32), preferred_element_type=jnp.float32)
    products = products.reshape(field_count, block_count, 2, wave_count)
    real_part = jnp.sum(cos_turn * products[:, :, 0] - sin_turn * products[:, :, 1], axis=1)
    imag_part = -jnp.sum(sin_turn * products[:, :, 0] + cos_turn * products[:, :, 1], axis=1)
    inverse_len = 1.0 / length.astype(jnp.float32)
    together = jnp.concatenate([real_part, imag_part], axis=0) * inverse_len
    resolved = 2 * wave_list < length
    together = jnp.where(resolved[None, :], together, 0.0)
    return together.T.astype(jnp.bfloat16)

def inverse_loop(fourier, length, wave_list, loop_width):
    block_count = loop_width // 128
    wave_count = wave_list.shape[0]
    field_count = fourier.shape[1] // 2
    inner_table, cos_turn, sin_turn = loop_tables(length, wave_list, block_count)
    doubling = jnp.where(wave_list == 0, 1.0, 2.0).astype(jnp.float32)
    real_part = fourier[:, :field_count].astype(jnp.float32).T * doubling
    imag_part = fourier[:, field_count:].astype(jnp.float32).T * doubling
    cosine_part = real_part[:, None, :] * cos_turn[None] - imag_part[:, None, :] * sin_turn[None]
    sine_part = -(real_part[:, None, :] * sin_turn[None] + imag_part[:, None, :] * cos_turn[None])
    combined = jnp.concatenate([cosine_part, sine_part], axis=2).astype(jnp.bfloat16)
    points = lax.dot_general(combined.reshape(field_count * block_count, 2 * wave_count).astype(jnp.float32), inner_table.astype(jnp.float32), (((1,), (1,)), ((), ())), preferred_element_type=jnp.float32)
    points = points.reshape(field_count, loop_width)
    inside = jnp.arange(loop_width, dtype=jnp.int32) < length
    return jnp.where(inside[None, :], points, 0.0).astype(jnp.bfloat16)

def semi_implicit(spectral, wave_values, vertical_modes, coupling, mode_rates):
    half_rows = spectral.shape[-2]
    level_count = vertical_modes.shape[0]
    parity = jnp.arange(2, dtype=jnp.int32)
    row_index = jnp.arange(half_rows, dtype=jnp.int32)
    degree = wave_values[..., None, None] + parity[:, None] + 2 * row_index[None, :]
    kept_rows = degree <= TRUNC
    spectral = jnp.where(kept_rows[..., None], spectral, 0.0)
    damping = (degree * (degree + 1)).astype(jnp.float32) / float(TRUNC * (TRUNC + 1))
    reshaped = spectral.reshape(spectral.shape[:-1] + (2, 2, level_count))
    divergence = reshaped[..., 0, :]
    pressure = reshaped[..., 1, :]
    factor_e = damping[..., None, None]
    right_side = divergence - implicit_step * factor_e * jnp.einsum('...l,kl->...k', pressure, coupling, precision=highest)
    in_modes = jnp.einsum('...l,lk->...k', right_side, vertical_modes, precision=highest)
    in_modes = in_modes / (1.0 + implicit_step * factor_e * mode_rates)
    new_div = jnp.einsum('...k,lk->...l', in_modes, vertical_modes, precision=highest)
    new_press = pressure - implicit_step * jnp.einsum('...l,kl->...k', new_div, coupling, precision=highest)
    updated = jnp.stack([new_div, new_press], axis=-2)
    return updated.reshape(spectral.shape).astype(jnp.bfloat16)

def reference(grid_in, legendre, gauss_weight, vertical_modes, coupling, mode_rates, loop_length, lat_order, wave_number):
    lat_count, field_count, loop_width = grid_in.shape
    half_count = lat_count // 2
    row_lengths = jnp.take(loop_length, lat_order)

    def forward_one(scan_item):
        return forward_loop(scan_item[0], scan_item[1], wave_number)
    fourier = lax.map(forward_one, (grid_in, row_lengths))
    row_of_lat = jnp.argsort(lat_order)
    northern = jnp.take(fourier, row_of_lat[:half_count], axis=0).astype(jnp.float32)
    southern = jnp.take(fourier, row_of_lat[::-1][:half_count], axis=0).astype(jnp.float32)
    weight = gauss_weight[:, None, None]
    even_part = (weight * (northern + southern)).astype(jnp.bfloat16)
    odd_part = (weight * (northern - southern)).astype(jnp.bfloat16)
    stacked = jnp.stack([even_part, odd_part], axis=0)
    per_wave = jnp.transpose(stacked, (2, 0, 1, 3))

    def wave_one(scan_item):
        table_block, columns, wave_value = scan_item
        table_wide = table_block.astype(jnp.float32)
        spectral = jnp.einsum('prj,pjc->prc', table_wide, columns.astype(jnp.float32), precision=highest)
        updated = semi_implicit(spectral, wave_value, vertical_modes, coupling, mode_rates)
        summed = jnp.einsum('prj,prc->pjc', table_wide, updated.astype(jnp.float32), precision=highest)
        northern_back = summed[0] + summed[1]
        southern_back = summed[0] - summed[1]
        by_lat = jnp.concatenate([northern_back, southern_back[::-1]], axis=0)
        resolved = 2 * wave_value < loop_length
        return jnp.where(resolved[:, None], by_lat, 0.0).astype(jnp.bfloat16)
    back_waves = lax.map(wave_one, (legendre, per_wave, wave_number))
    by_rows = jnp.take(back_waves, lat_order, axis=1)
    per_row = jnp.transpose(by_rows, (1, 0, 2))

    def inverse_one(scan_item):
        return inverse_loop(scan_item[0], scan_item[1], wave_number, loop_width)
    return lax.map(inverse_one, (per_row, row_lengths))
```

```python
import functools
import math

import jax
import jax.numpy as jnp
from jax import lax
from jax.experimental import pallas as pl
from jax.experimental.pallas import tpu as pltpu
from jax.sharding import PartitionSpec as P

TRUNC = 1279
STEP = 0.5
LANES = 128
MESH = pl.DeviceIdType.MESH
HIGHEST = lax.Precision.HIGHEST
F32 = jnp.float32
BF16 = jnp.bfloat16
I32 = jnp.int32

SIN_TERMS = [
    (-1.0) ** k * (2.0 * math.pi) ** (2 * k + 1) / math.factorial(2 * k + 1) for k in range(6)
]


def cos_turn(turn):
    near = turn - jnp.floor(turn + 0.5)
    z = 0.25 - jnp.abs(near)
    z2 = z * z
    total = jnp.full_like(z, SIN_TERMS[-1])
    for term in SIN_TERMS[-2::-1]:
        total = total * z2 + term
    return total * z


def iota(shape, dim):
    return lax.broadcasted_iota(I32, shape, dim)


def dot(a, b, dims=((1,), (0,)), precision=None):
    return lax.dot_general(a, b, (dims, ((), ())), precision=precision, preferred_element_type=F32)


def take_lanes(row8, index):
    return jnp.take_along_axis(row8, index, axis=1, mode="promise_in_bounds")


def for_peers(fn):
    me = lax.axis_index("band")
    x, y, c = me // 16, (me // 2) % 8, me % 2
    cores = [c, (c + 1) % 2]
    ys = [((y + dy) % 8) * 2 for dy in (4, 3, 5, 2, 6, 1, 7, 0)]

    def x_part(k):
        dx = 4 + ((k + 1) // 2) * (1 - 2 * (k % 2))
        return ((x + dx) % 8) * 16

    def most(k, carry):
        base = x_part(k)
        for at, part in enumerate(ys):
            fn(base + part + cores[1])
            if at < 7:
                fn(base + part + cores[0])
        return carry

    def rest(k, carry):
        fn(x_part(k) + ys[7] + cores[0])
        return carry

    lax.fori_loop(0, 8, most, 0)
    lax.fori_loop(0, 7, rest, 0)


def exchange(src, dst, send_sem, recv_sem, own_sem):
    me = lax.axis_index("band")

    def send(peer):
        pltpu.make_async_remote_copy(
            src.at[:, peer],
            dst.at[:, me],
            send_sem,
            recv_sem,
            device_id={"band": peer},
            device_id_type=MESH,
        ).start()

    for_peers(send)
    pltpu.make_async_copy(src.at[:, me], dst.at[:, me], own_sem).start()


def wait_exchange(src, dst, send_sem, recv_sem, own_sem, peers):
    me = lax.axis_index("band")
    some = pl.ds(0, peers)
    pltpu.make_async_copy(src.at[:, me], dst.at[:, me], own_sem).wait()
    pltpu.make_async_copy(src.at[:, some], dst.at[:, some], recv_sem).wait()


def wait_sent(src, dst, send_sem, peers):
    some = pl.ds(0, peers)
    pltpu.make_async_copy(src.at[:, some], dst.at[:, some], send_sem).wait()


def main_kernel(
    grid_hbm,
    leg_hbm,
    gw_hbm,
    vm_hbm,
    cp_hbm,
    mr_hbm,
    ll_hbm,
    lo_hbm,
    wn_hbm,
    a_ref,
    t_ref,
    gbuf,
    leg_v,
    gw_v,
    vm_v,
    cp_v,
    mr_v,
    ll_v,
    lo_v,
    wn_v,
    ll_s,
    lo_s,
    wn_s,
    base_c,
    base_s,
    turn_c,
    turn_s,
    facc,
    send1,
    recv1,
    send2,
    recv2,
    lhs,
    l2t,
    inv,
    kmix,
    vz,
    cz,
    rz,
    vpad,
    gpad,
    wall,
    pf,
    zf,
    loc_sem,
    grid_sem,
    send_sem,
    recv_sem,
    own_sem,
):
    band = lax.axis_index("band")
    fields, width = gbuf.shape
    levels = vm_v.shape[0]
    blocks = width // LANES
    lats = lo_v.shape[1]
    half, rows = leg_v.shape[1:]
    peers = lats - 1
    pairs = 2 * lats
    tiles = send1.shape[0]
    s1 = send1.reshape(tiles, pairs, LANES)
    r1 = recv1.reshape(tiles, pairs, LANES)
    s2 = send2.reshape(tiles, pairs, LANES)
    r2 = recv2.reshape(tiles, pairs, LANES)

    small = [
        (lo_hbm, lo_s),
        (ll_hbm, ll_s),
        (wn_hbm, wn_v),
        (wn_hbm, wn_s),
        (lo_hbm, lo_v),
        (ll_hbm, ll_v),
        (gw_hbm, gw_v),
        (mr_hbm, mr_v),
        (vm_hbm, vm_v),
        (cp_hbm, cp_v),
        (leg_hbm, leg_v),
    ]
    small = [pltpu.make_async_copy(s, d, loc_sem.at[k]) for k, (s, d) in enumerate(small)]
    for copy in small[:3]:
        copy.start()
    chunks = [(k, min(4, blocks - k)) for k in range(0, blocks, 4)]
    loads = []
    for n, (k, count) in enumerate(chunks):
        part = pl.ds(k * LANES, count * LANES)
        loads.append(pltpu.make_async_copy(grid_hbm.at[:, part], gbuf.at[:, part], grid_sem.at[n]))
        loads[-1].start()
    for copy in small[3:]:
        copy.start()

    barrier = pltpu.get_barrier_semaphore()
    for_peers(
        lambda peer: pl.semaphore_signal(
            barrier, inc=1, device_id={"band": peer}, device_id_type=MESH
        )
    )
    facc[fields:, :] = jnp.zeros((facc.shape[0] - fields, pairs), F32)

    for copy in small[:3]:
        copy.wait()
    length = ll_s[0, lo_s[0, band]]
    lane = iota((8, LANES), 1)
    waves8 = jnp.broadcast_to(wn_v[...], (8, LANES))
    waves = jnp.concatenate(
        [take_lanes(waves8, lane // 2 + k * (LANES // 2)) for k in range(2)], axis=1
    )[0:1].astype(F32)
    quarter = (iota((1, pairs), 1) % 2).astype(F32) * 0.25
    length_row = jnp.full((1, pairs), length.astype(F32))
    inv_length = 1.0 / length_row

    def turns(count, stride):
        x = (iota((count, pairs), 0) * stride).astype(F32) * waves
        return (x - jnp.floor(x * inv_length) * length_row) * inv_length

    fine = turns(8, 1) + quarter
    fine_c, fine_s = cos_turn(fine), cos_turn(fine - 0.25)
    mid = turns(16, 8)
    mid_c, mid_s = cos_turn(mid), cos_turn(mid - 0.25)
    for k in range(16):
        c, s = mid_c[k : k + 1], mid_s[k : k + 1]
        base_c[8 * k : 8 * k + 8, :] = c * fine_c - s * fine_s
        base_s[8 * k : 8 * k + 8, :] = s * fine_c + c * fine_s
    far = turns(turn_c.shape[0], LANES)
    turn_c[...] = cos_turn(far)
    turn_s[...] = cos_turn(far - 0.25)
    place = iota((LANES, pairs), 0)
    acc = None
    for n, (k, count) in enumerate(chunks):
        for a in range(k, k + count):
            block = turn_c[a : a + 1, :] * base_c[...] - turn_s[a : a + 1, :] * base_s[...]
            block = jnp.where(place < length - a * LANES, block, 0.0)
            t_ref[a * LANES : (a + 1) * LANES, :] = block.astype(BF16)
        loads[n].wait()
        part = pl.ds(k * LANES, count * LANES)
        product = dot(gbuf[:, part], t_ref[part, :])
        acc = product if acc is None else acc + product
    scale = jnp.where(2.0 * waves < length_row, inv_length, 0.0)
    facc[:fields, :] = acc * scale
    for t in range(tiles):
        s1[t] = facc[t * LANES : (t + 1) * LANES, :].T.astype(BF16)

    pl.semaphore_wait(barrier, peers)
    exchange(send1, recv1, send_sem.at[0], recv_sem.at[0], own_sem.at[0])

    for copy in small[3:]:
        copy.wait()
    wave = wn_s[0, band]
    lat = lo_v[...]
    north = lat < half
    lat_row = jnp.where(north, lat, lats - 1 - lat)
    select = jnp.where(iota((half, lats), 0) == lat_row, 1.0, 0.0)
    sign = jnp.where(north, 1.0, -1.0)
    weight = dot(jnp.broadcast_to(gw_v[...], (8, half)), select, precision=HIGHEST)[0:1]
    select = select.astype(BF16)
    lat8 = jnp.broadcast_to(lat, (8, lats))
    length8 = take_lanes(jnp.broadcast_to(ll_v[...], (8, lats)), lat8)
    length_col = jnp.broadcast_to(length8[0:1].astype(F32), (lats, lats)).T
    lat_col = jnp.broadcast_to(lat.astype(F32), (lats, lats)).T
    north_col = lat_col < half
    sign_col = jnp.where(north_col, 1.0, -1.0)[:, 0:1]
    place_col = jnp.where(north_col, lat_col, lats - 1.0 - lat_col)[:, :half]
    select_t = jnp.where(iota((lats, half), 1).astype(F32) == place_col, 1.0, 0.0).astype(BF16)
    doubling = jnp.where(jnp.full((lats, lats), wave) == 0, 1.0, 2.0)
    wave_f = jnp.full((lats, lats), wave).astype(F32)
    keep_col = jnp.where(2.0 * wave_f < length_col, doubling, 0.0)[:, 0:1]

    rz[...] = jnp.zeros(rz.shape, F32)
    rz[0:1, :levels] = mr_v[...]
    rates = rz[0:1, :]
    for p in range(2):
        table = leg_v[p]
        span = slice(p * rows, (p + 1) * rows)
        degree = iota((rows, LANES), 0) * 2 + (wave + p)
        energy = (degree * (degree + 1)).astype(F32) * (STEP / float(TRUNC * (TRUNC + 1)))
        gain = weight if p == 0 else weight * sign
        own = jnp.where(degree <= TRUNC, dot(table, select, ((0,), (0,))) * gain, 0.0)
        lhs[span, :LANES] = own.astype(BF16)
        lhs[span, LANES:] = (own * -energy).astype(BF16)
        for t in range(2):
            inv[span, t * LANES : (t + 1) * LANES] = 1.0 / (
                1.0 + energy * rates[:, t * LANES : (t + 1) * LANES]
            )
        gain_col = keep_col if p == 0 else keep_col * sign_col
        l2t[:, span] = (dot(select_t, table) * gain_col).astype(BF16)
    mix = dot(l2t[...], lhs[:, :LANES]).astype(BF16)
    spread = []
    for q in range(2):
        each = jnp.where(iota((pairs, lats), 0) == iota((pairs, lats), 1) * 2 + q, 1.0, 0.0)
        each = each.astype(BF16)
        spread.append(dot(dot(each, mix).astype(BF16), each, ((1,), (1,))))
    kmix[...] = (spread[0] + spread[1]).astype(BF16)

    vz[...] = jnp.zeros(vz.shape, F32)
    cz[...] = jnp.zeros(cz.shape, F32)
    vz[:levels, :levels] = vm_v[...]
    cz[:levels, :levels] = cp_v[...]
    modes, couple = vz[...], cz[...]
    square = modes.shape
    vpad[...] = modes.astype(BF16)
    gap = levels - LANES
    shift = jnp.where(iota(square, 0) == iota(square, 1) + gap, 1.0, 0.0)
    moved = dot(shift, couple, ((1,), (1,)), precision=HIGHEST)
    gpad[...] = dot(moved, modes, precision=HIGHEST).astype(BF16)
    wide = (square[0], tiles * LANES)
    shift = jnp.where(iota(wide, 1) == iota(wide, 0) + levels, 1.0, 0.0)
    same = jnp.where(iota(wide, 1) == iota(wide, 0), 1.0, 0.0)
    spread_out = same - STEP * dot(couple, shift, ((0,), (0,)), precision=HIGHEST)
    wall[...] = dot(modes, spread_out, ((0,), (0,)), precision=HIGHEST).astype(BF16)

    wait_exchange(send1, recv1, send_sem.at[0], recv_sem.at[0], own_sem.at[0], peers)
    f0, f1, f2 = r1[0], r1[1], r1[2]
    in_d = dot(jnp.concatenate([f0, f1], axis=1), vpad[...])
    in_p = dot(jnp.concatenate([f1, f2], axis=1), gpad[...])
    for t in range(2):
        pf[t] = in_d[:, t * LANES : (t + 1) * LANES]
        pf[2 + t] = in_p[:, t * LANES : (t + 1) * LANES]
    only_p = jnp.where(iota(f1.shape, 1) < gap, 0.0, 1.0).astype(BF16)
    f1 = f1 * only_p
    own_p = dot(kmix[...], jnp.concatenate([f1, f2], axis=1))
    for q in range(2):
        part = pl.ds(q, lats, stride=2)
        rhs = jnp.concatenate(
            [
                jnp.concatenate([pf[0, part, :], pf[1, part, :]], axis=1),
                jnp.concatenate([pf[2, part, :], pf[3, part, :]], axis=1),
            ],
            axis=0,
        ).astype(BF16)
        total = None
        for k in range(0, 2 * rows, 2 * LANES):
            span = slice(k, k + 2 * LANES)
            solved = (dot(lhs[span, :], rhs) * inv[span, :]).astype(BF16)
            product = dot(l2t[:, span], solved)
            total = product if total is None else total + product
        for t in range(2):
            zf[t, part, :] = total[:, t * LANES : (t + 1) * LANES]
    back = jnp.concatenate([zf[0], zf[1]], axis=1).astype(BF16)
    out = dot(back, wall[...])
    s2[0] = out[:, :LANES].astype(BF16)
    s2[1] = (out[:, LANES : 2 * LANES] + own_p[:, :LANES]).astype(BF16)
    s2[2] = (out[:, 2 * LANES :] + own_p[:, LANES:]).astype(BF16)

    exchange(send2, recv2, send_sem.at[1], recv_sem.at[1], own_sem.at[1])
    wait_sent(send1, recv1, send_sem.at[0], peers)
    wait_exchange(send2, recv2, send_sem.at[1], recv_sem.at[1], own_sem.at[1], peers)
    for t in range(tiles):
        a_ref[t * LANES : (t + 1) * LANES, :] = r2[t].astype(F32).T.astype(BF16)
    wait_sent(send2, recv2, send_sem.at[1], peers)


def inverse_kernel(a_ref, t_ref, out_hbm, obuf, sem):
    fields, width = obuf.shape
    step = 4 * LANES
    copies = []
    for n, k in enumerate(range(0, width, step)):
        part = pl.ds(k, min(step, width - k))
        obuf[:, part] = dot(a_ref[:fields, :], t_ref[part, :], ((1,), (1,))).astype(BF16)
        copies.append(pltpu.make_async_copy(obuf.at[:, part], out_hbm.at[:, part], sem.at[n]))
        copies[-1].start()
    for copy in copies:
        copy.wait()


def per_device(grid_in, legendre, gauss_weight, vertical_modes, coupling, mode_rates, loop_length, lat_order, wave_number):
    fields, width = grid_in.shape[1:]
    rows, half = legendre.shape[2:]
    levels = vertical_modes.shape[0]
    lats = lat_order.shape[0]
    pairs = 2 * lats
    tiles = -(-fields // LANES)
    blocks = width // LANES
    operands = [
        grid_in.reshape(fields, width),
        jnp.swapaxes(legendre.reshape(2, rows, half), 1, 2),
        gauss_weight.reshape(1, half),
        vertical_modes,
        coupling,
        mode_rates.reshape(1, levels),
        loop_length.reshape(1, lats),
        lat_order.reshape(1, lats),
        wave_number.reshape(1, lats),
    ]
    hbm = pl.BlockSpec(memory_space=pltpu.HBM)
    vmem = pl.BlockSpec(memory_space=pltpu.VMEM)
    dma = pltpu.SemaphoreType.DMA
    a_mat, table = pl.pallas_call(
        main_kernel,
        out_shape=(
            pltpu.VMEM((tiles * LANES, pairs), BF16),
            pltpu.VMEM((width, pairs), BF16),
        ),
        in_specs=[hbm] * 9,
        out_specs=(vmem, vmem),
        scratch_shapes=[
            pltpu.VMEM((fields, width), BF16),
            pltpu.VMEM((2, half, rows), BF16),
            pltpu.VMEM((1, half), F32),
            pltpu.VMEM((levels, levels), F32),
            pltpu.VMEM((levels, levels), F32),
            pltpu.VMEM((1, levels), F32),
            pltpu.VMEM((1, lats), I32),
            pltpu.VMEM((1, lats), I32),
            pltpu.VMEM((1, lats), I32),
            pltpu.SMEM((1, lats), I32),
            pltpu.SMEM((1, lats), I32),
            pltpu.SMEM((1, lats), I32),
            pltpu.VMEM((LANES, pairs), F32),
            pltpu.VMEM((LANES, pairs), F32),
            pltpu.VMEM((-(-blocks // 8) * 8, pairs), F32),
            pltpu.VMEM((-(-blocks // 8) * 8, pairs), F32),
            pltpu.VMEM((tiles * LANES, pairs), F32),
            pltpu.VMEM((tiles, lats, 2, LANES), BF16),
            pltpu.VMEM((tiles, lats, 2, LANES), BF16),
            pltpu.VMEM((tiles, lats, 2, LANES), BF16),
            pltpu.VMEM((tiles, lats, 2, LANES), BF16),
            pltpu.VMEM((2 * rows, 2 * LANES), BF16),
            pltpu.VMEM((lats, 2 * rows), BF16),
            pltpu.VMEM((2 * rows, 2 * LANES), F32),
            pltpu.VMEM((pairs, pairs), BF16),
            pltpu.VMEM((2 * LANES, 2 * LANES), F32),
            pltpu.VMEM((2 * LANES, 2 * LANES), F32),
            pltpu.VMEM((8, 2 * LANES), F32),
            pltpu.VMEM((2 * LANES, 2 * LANES), BF16),
            pltpu.VMEM((2 * LANES, 2 * LANES), BF16),
            pltpu.VMEM((2 * LANES, tiles * LANES), BF16),
            pltpu.VMEM((4, pairs, LANES), F32),
            pltpu.VMEM((2, pairs, LANES), F32),
            dma((11,)),
            dma((-(-blocks // 4),)),
            dma((2,)),
            dma((2,)),
            dma((2,)),
        ],
        compiler_params=pltpu.CompilerParams(
            collective_id=1, has_side_effects=True, vmem_limit_bytes=40 * 2**20
        ),
        name="spectral_step",
    )(*[pltpu.with_memory_space_constraint(each, pltpu.HBM) for each in operands])
    a_mat = pltpu.with_memory_space_constraint(a_mat, pltpu.VMEM)
    table = pltpu.with_memory_space_constraint(table, pltpu.VMEM)
    points = pl.pallas_call(
        inverse_kernel,
        out_shape=jax.ShapeDtypeStruct((fields, width), BF16),
        in_specs=[vmem, vmem],
        out_specs=hbm,
        scratch_shapes=[pltpu.VMEM((fields, width), BF16), dma((-(-blocks // 4),))],
        compiler_params=pltpu.CompilerParams(vmem_limit_bytes=16 * 2**20),
        name="inverse_loop",
    )(a_mat, table)
    return points.reshape(grid_in.shape)


def solution(mesh):
    whole = P(("member", "band"), None, None)
    in_specs = (whole, P("band", None, None, None)) + (P(),) * 7
    return jax.shard_map(per_device, mesh=mesh, in_specs=in_specs, out_specs=whole, check_vma=False)
```

```python
import functools
import math

import jax
import jax.numpy as jnp
from jax import lax
from jax.experimental import pallas as pl
from jax.experimental.pallas import tpu as pltpu
from jax.sharding import PartitionSpec as P

TRUNC = 1279
STEP = 0.5
LANES = 128
MESH = pl.DeviceIdType.MESH
HIGHEST = lax.Precision.HIGHEST
F32 = jnp.float32
BF16 = jnp.bfloat16
I32 = jnp.int32

SIN_TERMS = [
    (-1.0) ** k * (2.0 * math.pi) ** (2 * k + 1) / math.factorial(2 * k + 1) for k in range(6)
]


def cos_turn(turn):
    near = turn - jnp.floor(turn + 0.5)
    z = 0.25 - jnp.abs(near)
    z2 = z * z
    total = jnp.full_like(z, SIN_TERMS[-1])
    for term in SIN_TERMS[-2::-1]:
        total = total * z2 + term
    return total * z


def iota(shape, dim):
    return lax.broadcasted_iota(I32, shape, dim)


def dot(a, b, dims=((1,), (0,)), precision=None):
    return lax.dot_general(a, b, (dims, ((), ())), precision=precision, preferred_element_type=F32)


def take_lanes(row8, index):
    return jnp.take_along_axis(row8, index, axis=1, mode="promise_in_bounds")


FAR_FIRST = (4, 3, 5, 2, 6, 1, 7, 0)


def far_first(k):
    return 4 + ((k + 1) // 2) * (1 - 2 * (k % 2))


def place():
    me = lax.axis_index("band")
    return me // 16, (me // 2) % 8, me % 2


def at_place(x, y, c):
    return (x % 8) * 16 + (y % 8) * 2 + c % 2


def signal(sem, peer):
    pl.semaphore_signal(sem, inc=1, device_id={"band": peer}, device_id_type=MESH)


def greet(barrier):
    x, y, c = place()
    for dx in FAR_FIRST:
        for dc in (1, 0):
            if dx or dc:
                signal(barrier, at_place(x + dx, y, c + dc))
    for dy in FAR_FIRST[:7]:
        signal(barrier, at_place(x, y + dy, c))


GREETINGS = 22


def announce(ready):
    x, y, c = place()
    for k, dy in enumerate(FAR_FIRST[:7]):
        signal(ready.at[FAR_FIRST.index((8 - dy) % 8)], at_place(x, y + dy, c))


def exchange(src, dst, send_sem, recv_sem, own_sem, ready=None):
    me = lax.axis_index("band")
    x, y, c = place()
    parts = [((x + dx) % 8) * 16 for dx in FAR_FIRST]
    cores = [(c + 1) % 2, c]

    def send(peer):
        pltpu.make_async_remote_copy(
            src.at[:, peer],
            dst.at[:, me],
            send_sem,
            recv_sem,
            device_id={"band": peer},
            device_id_type=MESH,
        ).start()

    def column(k, carry):
        if ready is not None:
            pl.semaphore_wait(ready.at[k], 1)
        base = ((y + far_first(k)) % 8) * 2
        for part in parts:
            for core in cores:
                send(base + part + core)
        return carry

    lax.fori_loop(0, 7, column, 0)
    for n, part in enumerate(parts):
        for core in cores[: 2 if n < 7 else 1]:
            send(y * 2 + part + core)
    pltpu.make_async_copy(src.at[:, me], dst.at[:, me], own_sem).start()


def wait_exchange(src, dst, send_sem, recv_sem, own_sem, peers):
    me = lax.axis_index("band")
    some = pl.ds(0, peers)
    pltpu.make_async_copy(src.at[:, me], dst.at[:, me], own_sem).wait()
    pltpu.make_async_copy(src.at[:, some], dst.at[:, some], recv_sem).wait()


def wait_sent(src, dst, send_sem, peers):
    some = pl.ds(0, peers)
    pltpu.make_async_copy(src.at[:, some], dst.at[:, some], send_sem).wait()


def main_kernel(
    grid_hbm,
    leg_hbm,
    gw_hbm,
    vm_hbm,
    cp_hbm,
    mr_hbm,
    ll_hbm,
    lo_hbm,
    wn_hbm,
    a_ref,
    t_ref,
    gbuf,
    leg_v,
    gw_v,
    vm_v,
    cp_v,
    mr_v,
    ll_v,
    lo_v,
    wn_v,
    ll_s,
    lo_s,
    wn_s,
    base_c,
    base_s,
    turn_c,
    turn_s,
    facc,
    send1,
    recv1,
    send2,
    recv2,
    lhs,
    l2t,
    inv,
    kmix,
    vz,
    cz,
    rz,
    vpad,
    gpad,
    wall,
    pf,
    zf,
    loc_sem,
    grid_sem,
    send_sem,
    recv_sem,
    own_sem,
    ready,
):
    band = lax.axis_index("band")
    fields, width = gbuf.shape
    levels = vm_v.shape[0]
    blocks = width // LANES
    lats = lo_v.shape[1]
    half, rows = leg_v.shape[1:]
    peers = lats - 1
    pairs = 2 * lats
    tiles = send1.shape[0]
    s1 = send1.reshape(tiles, pairs, LANES)
    r1 = recv1.reshape(tiles, pairs, LANES)
    s2 = send2.reshape(tiles, pairs, LANES)
    r2 = recv2.reshape(tiles, pairs, LANES)

    small = [
        (lo_hbm, lo_s),
        (ll_hbm, ll_s),
        (wn_hbm, wn_v),
        (wn_hbm, wn_s),
        (lo_hbm, lo_v),
        (ll_hbm, ll_v),
        (gw_hbm, gw_v),
        (mr_hbm, mr_v),
        (vm_hbm, vm_v),
        (cp_hbm, cp_v),
        (leg_hbm, leg_v),
    ]
    small = [pltpu.make_async_copy(s, d, loc_sem.at[k]) for k, (s, d) in enumerate(small)]
    for copy in small[:3]:
        copy.start()
    chunks = [(k, min(4, blocks - k)) for k in range(0, blocks, 4)]
    loads = []
    for n, (k, count) in enumerate(chunks):
        part = pl.ds(k * LANES, count * LANES)
        loads.append(pltpu.make_async_copy(grid_hbm.at[:, part], gbuf.at[:, part], grid_sem.at[n]))
        loads[-1].start()
    for copy in small[3:]:
        copy.start()

    barrier = pltpu.get_barrier_semaphore()
    greet(barrier)
    facc[fields:, :] = jnp.zeros((facc.shape[0] - fields, pairs), F32)

    for copy in small[:3]:
        copy.wait()
    length = ll_s[0, lo_s[0, band]]
    lane = iota((8, LANES), 1)
    waves8 = jnp.broadcast_to(wn_v[...], (8, LANES))
    waves = jnp.concatenate(
        [take_lanes(waves8, lane // 2 + k * (LANES // 2)) for k in range(2)], axis=1
    )[0:1].astype(F32)
    quarter = (iota((1, pairs), 1) % 2).astype(F32) * 0.25
    length_row = jnp.full((1, pairs), length.astype(F32))
    inv_length = 1.0 / length_row

    def turns(count, stride):
        x = (iota((count, pairs), 0) * stride).astype(F32) * waves
        return (x - jnp.floor(x * inv_length) * length_row) * inv_length

    fine = turns(8, 1) + quarter
    fine_c, fine_s = cos_turn(fine), cos_turn(fine - 0.25)
    mid = turns(16, 8)
    mid_c, mid_s = cos_turn(mid), cos_turn(mid - 0.25)
    for k in range(16):
        c, s = mid_c[k : k + 1], mid_s[k : k + 1]
        base_c[8 * k : 8 * k + 8, :] = c * fine_c - s * fine_s
        base_s[8 * k : 8 * k + 8, :] = s * fine_c + c * fine_s
    far = turns(turn_c.shape[0], LANES)
    turn_c[...] = cos_turn(far)
    turn_s[...] = cos_turn(far - 0.25)
    within = iota((LANES, pairs), 0)
    acc = None
    for n, (k, count) in enumerate(chunks):
        for a in range(k, k + count):
            block = turn_c[a : a + 1, :] * base_c[...] - turn_s[a : a + 1, :] * base_s[...]
            block = jnp.where(within < length - a * LANES, block, 0.0)
            t_ref[a * LANES : (a + 1) * LANES, :] = block.astype(BF16)
        loads[n].wait()
        part = pl.ds(k * LANES, count * LANES)
        product = dot(gbuf[:, part], t_ref[part, :])
        acc = product if acc is None else acc + product
    scale = jnp.where(2.0 * waves < length_row, inv_length, 0.0)
    facc[:fields, :] = acc * scale
    for t in range(tiles):
        s1[t] = facc[t * LANES : (t + 1) * LANES, :].T.astype(BF16)

    pl.semaphore_wait(barrier, GREETINGS)
    announce(ready)
    exchange(send1, recv1, send_sem.at[0], recv_sem.at[0], own_sem.at[0], ready)

    for copy in small[3:]:
        copy.wait()
    wave = wn_s[0, band]
    lat = lo_v[...]
    north = lat < half
    lat_row = jnp.where(north, lat, lats - 1 - lat)
    select = jnp.where(iota((half, lats), 0) == lat_row, 1.0, 0.0)
    sign = jnp.where(north, 1.0, -1.0)
    weight = dot(jnp.broadcast_to(gw_v[...], (8, half)), select, precision=HIGHEST)[0:1]
    select = select.astype(BF16)
    lat8 = jnp.broadcast_to(lat, (8, lats))
    length8 = take_lanes(jnp.broadcast_to(ll_v[...], (8, lats)), lat8)
    length_col = jnp.broadcast_to(length8[0:1].astype(F32), (lats, lats)).T
    lat_col = jnp.broadcast_to(lat.astype(F32), (lats, lats)).T
    north_col = lat_col < half
    sign_col = jnp.where(north_col, 1.0, -1.0)[:, 0:1]
    place_col = jnp.where(north_col, lat_col, lats - 1.0 - lat_col)[:, :half]
    select_t = jnp.where(iota((lats, half), 1).astype(F32) == place_col, 1.0, 0.0).astype(BF16)
    doubling = jnp.where(jnp.full((lats, lats), wave) == 0, 1.0, 2.0)
    wave_f = jnp.full((lats, lats), wave).astype(F32)
    keep_col = jnp.where(2.0 * wave_f < length_col, doubling, 0.0)[:, 0:1]

    rz[...] = jnp.zeros(rz.shape, F32)
    rz[0:1, :levels] = mr_v[...]
    rates = rz[0:1, :]
    for p in range(2):
        table = leg_v[p]
        span = slice(p * rows, (p + 1) * rows)
        degree = iota((rows, LANES), 0) * 2 + (wave + p)
        energy = (degree * (degree + 1)).astype(F32) * (STEP / float(TRUNC * (TRUNC + 1)))
        gain = weight if p == 0 else weight * sign
        own = jnp.where(degree <= TRUNC, dot(table, select, ((0,), (0,))) * gain, 0.0)
        lhs[span, :LANES] = own.astype(BF16)
        lhs[span, LANES:] = (own * -energy).astype(BF16)
        for t in range(2):
            inv[span, t * LANES : (t + 1) * LANES] = 1.0 / (
                1.0 + energy * rates[:, t * LANES : (t + 1) * LANES]
            )
        gain_col = keep_col if p == 0 else keep_col * sign_col
        l2t[:, span] = (dot(select_t, table) * gain_col).astype(BF16)
    mix = dot(l2t[...], lhs[:, :LANES]).astype(BF16)
    spread = []
    for q in range(2):
        each = jnp.where(iota((pairs, lats), 0) == iota((pairs, lats), 1) * 2 + q, 1.0, 0.0)
        each = each.astype(BF16)
        spread.append(dot(dot(each, mix).astype(BF16), each, ((1,), (1,))))
    kmix[...] = (spread[0] + spread[1]).astype(BF16)

    vz[...] = jnp.zeros(vz.shape, F32)
    cz[...] = jnp.zeros(cz.shape, F32)
    vz[:levels, :levels] = vm_v[...]
    cz[:levels, :levels] = cp_v[...]
    modes, couple = vz[...], cz[...]
    square = modes.shape
    vpad[...] = modes.astype(BF16)
    gap = levels - LANES
    shift = jnp.where(iota(square, 0) == iota(square, 1) + gap, 1.0, 0.0)
    moved = dot(shift, couple, ((1,), (1,)), precision=HIGHEST)
    gpad[...] = dot(moved, modes, precision=HIGHEST).astype(BF16)
    wide = (square[0], tiles * LANES)
    shift = jnp.where(iota(wide, 1) == iota(wide, 0) + levels, 1.0, 0.0)
    same = jnp.where(iota(wide, 1) == iota(wide, 0), 1.0, 0.0)
    spread_out = same - STEP * dot(couple, shift, ((0,), (0,)), precision=HIGHEST)
    wall[...] = dot(modes, spread_out, ((0,), (0,)), precision=HIGHEST).astype(BF16)

    wait_exchange(send1, recv1, send_sem.at[0], recv_sem.at[0], own_sem.at[0], peers)
    f0, f1, f2 = r1[0], r1[1], r1[2]
    in_d = dot(jnp.concatenate([f0, f1], axis=1), vpad[...])
    in_p = dot(jnp.concatenate([f1, f2], axis=1), gpad[...])
    for t in range(2):
        pf[t] = in_d[:, t * LANES : (t + 1) * LANES]
        pf[2 + t] = in_p[:, t * LANES : (t + 1) * LANES]
    only_p = jnp.where(iota(f1.shape, 1) < gap, 0.0, 1.0).astype(BF16)
    f1 = f1 * only_p
    own_p = dot(kmix[...], jnp.concatenate([f1, f2], axis=1))
    for q in range(2):
        part = pl.ds(q, lats, stride=2)
        rhs = jnp.concatenate(
            [
                jnp.concatenate([pf[0, part, :], pf[1, part, :]], axis=1),
                jnp.concatenate([pf[2, part, :], pf[3, part, :]], axis=1),
            ],
            axis=0,
        ).astype(BF16)
        total = None
        for k in range(0, 2 * rows, 2 * LANES):
            span = slice(k, k + 2 * LANES)
            solved = (dot(lhs[span, :], rhs) * inv[span, :]).astype(BF16)
            product = dot(l2t[:, span], solved)
            total = product if total is None else total + product
        for t in range(2):
            zf[t, part, :] = total[:, t * LANES : (t + 1) * LANES]
    back = jnp.concatenate([zf[0], zf[1]], axis=1).astype(BF16)
    out = dot(back, wall[...])
    s2[0] = out[:, :LANES].astype(BF16)
    s2[1] = (out[:, LANES : 2 * LANES] + own_p[:, :LANES]).astype(BF16)
    s2[2] = (out[:, 2 * LANES :] + own_p[:, LANES:]).astype(BF16)

    exchange(send2, recv2, send_sem.at[1], recv_sem.at[1], own_sem.at[1])
    wait_sent(send1, recv1, send_sem.at[0], peers)
    wait_exchange(send2, recv2, send_sem.at[1], recv_sem.at[1], own_sem.at[1], peers)
    for t in range(tiles):
        a_ref[t * LANES : (t + 1) * LANES, :] = r2[t].astype(F32).T.astype(BF16)
    wait_sent(send2, recv2, send_sem.at[1], peers)


def inverse_kernel(a_ref, t_ref, out_hbm, obuf, sem):
    fields, width = obuf.shape
    step = 4 * LANES
    copies = []
    for n, k in enumerate(range(0, width, step)):
        part = pl.ds(k, min(step, width - k))
        obuf[:, part] = dot(a_ref[:fields, :], t_ref[part, :], ((1,), (1,))).astype(BF16)
        copies.append(pltpu.make_async_copy(obuf.at[:, part], out_hbm.at[:, part], sem.at[n]))
        copies[-1].start()
    for copy in copies:
        copy.wait()


def per_device(grid_in, legendre, gauss_weight, vertical_modes, coupling, mode_rates, loop_length, lat_order, wave_number):
    fields, width = grid_in.shape[1:]
    rows, half = legendre.shape[2:]
    levels = vertical_modes.shape[0]
    lats = lat_order.shape[0]
    pairs = 2 * lats
    tiles = -(-fields // LANES)
    blocks = width // LANES
    operands = [
        grid_in.reshape(fields, width),
        jnp.swapaxes(legendre.reshape(2, rows, half), 1, 2),
        gauss_weight.reshape(1, half),
        vertical_modes,
        coupling,
        mode_rates.reshape(1, levels),
        loop_length.reshape(1, lats),
        lat_order.reshape(1, lats),
        wave_number.reshape(1, lats),
    ]
    hbm = pl.BlockSpec(memory_space=pltpu.HBM)
    vmem = pl.BlockSpec(memory_space=pltpu.VMEM)
    dma = pltpu.SemaphoreType.DMA
    a_mat, table = pl.pallas_call(
        main_kernel,
        out_shape=(
            pltpu.VMEM((tiles * LANES, pairs), BF16),
            pltpu.VMEM((width, pairs), BF16),
        ),
        in_specs=[hbm] * 9,
        out_specs=(vmem, vmem),
        scratch_shapes=[
            pltpu.VMEM((fields, width), BF16),
            pltpu.VMEM((2, half, rows), BF16),
            pltpu.VMEM((1, half), F32),
            pltpu.VMEM((levels, levels), F32),
            pltpu.VMEM((levels, levels), F32),
            pltpu.VMEM((1, levels), F32),
            pltpu.VMEM((1, lats), I32),
            pltpu.VMEM((1, lats), I32),
            pltpu.VMEM((1, lats), I32),
            pltpu.SMEM((1, lats), I32),
            pltpu.SMEM((1, lats), I32),
            pltpu.SMEM((1, lats), I32),
            pltpu.VMEM((LANES, pairs), F32),
            pltpu.VMEM((LANES, pairs), F32),
            pltpu.VMEM((-(-blocks // 8) * 8, pairs), F32),
            pltpu.VMEM((-(-blocks // 8) * 8, pairs), F32),
            pltpu.VMEM((tiles * LANES, pairs), F32),
            pltpu.VMEM((tiles, lats, 2, LANES), BF16),
            pltpu.VMEM((tiles, lats, 2, LANES), BF16),
            pltpu.VMEM((tiles, lats, 2, LANES), BF16),
            pltpu.VMEM((tiles, lats, 2, LANES), BF16),
            pltpu.VMEM((2 * rows, 2 * LANES), BF16),
            pltpu.VMEM((lats, 2 * rows), BF16),
            pltpu.VMEM((2 * rows, 2 * LANES), F32),
            pltpu.VMEM((pairs, pairs), BF16),
            pltpu.VMEM((2 * LANES, 2 * LANES), F32),
            pltpu.VMEM((2 * LANES, 2 * LANES), F32),
            pltpu.VMEM((8, 2 * LANES), F32),
            pltpu.VMEM((2 * LANES, 2 * LANES), BF16),
            pltpu.VMEM((2 * LANES, 2 * LANES), BF16),
            pltpu.VMEM((2 * LANES, tiles * LANES), BF16),
            pltpu.VMEM((4, pairs, LANES), F32),
            pltpu.VMEM((2, pairs, LANES), F32),
            dma((11,)),
            dma((-(-blocks // 4),)),
            dma((2,)),
            dma((2,)),
            dma((2,)),
            pltpu.SemaphoreType.REGULAR((7,)),
        ],
        compiler_params=pltpu.CompilerParams(
            collective_id=1, has_side_effects=True, vmem_limit_bytes=40 * 2**20
        ),
        name="spectral_step",
    )(*[pltpu.with_memory_space_constraint(each, pltpu.HBM) for each in operands])
    a_mat = pltpu.with_memory_space_constraint(a_mat, pltpu.VMEM)
    table = pltpu.with_memory_space_constraint(table, pltpu.VMEM)
    points = pl.pallas_call(
        inverse_kernel,
        out_shape=jax.ShapeDtypeStruct((fields, width), BF16),
        in_specs=[vmem, vmem],
        out_specs=hbm,
        scratch_shapes=[pltpu.VMEM((fields, width), BF16), dma((-(-blocks // 4),))],
        compiler_params=pltpu.CompilerParams(vmem_limit_bytes=16 * 2**20),
        name="inverse_loop",
    )(a_mat, table)
    return points.reshape(grid_in.shape)


def solution(mesh):
    whole = P(("member", "band"), None, None)
    in_specs = (whole, P("band", None, None, None)) + (P(),) * 7
    return jax.shard_map(per_device, mesh=mesh, in_specs=in_specs, out_specs=whole, check_vma=False)
```

```python
import functools
import math

import jax
import jax.numpy as jnp
from jax import lax
from jax.experimental import pallas as pl
from jax.experimental.pallas import tpu as pltpu
from jax.sharding import PartitionSpec as P

TRUNC = 1279
STEP = 0.5
LANES = 128
MESH = pl.DeviceIdType.MESH
HIGHEST = lax.Precision.HIGHEST
F32 = jnp.float32
BF16 = jnp.bfloat16
I32 = jnp.int32

SIN_TERMS = [
    (-1.0) ** k * (2.0 * math.pi) ** (2 * k + 1) / math.factorial(2 * k + 1) for k in range(6)
]


def cos_turn(turn):
    near = turn - jnp.floor(turn + 0.5)
    z = 0.25 - jnp.abs(near)
    z2 = z * z
    total = jnp.full_like(z, SIN_TERMS[-1])
    for term in SIN_TERMS[-2::-1]:
        total = total * z2 + term
    return total * z


def iota(shape, dim):
    return lax.broadcasted_iota(I32, shape, dim)


def dot(a, b, dims=((1,), (0,)), precision=None):
    return lax.dot_general(a, b, (dims, ((), ())), precision=precision, preferred_element_type=F32)


def take_lanes(row8, index):
    return jnp.take_along_axis(row8, index, axis=1, mode="promise_in_bounds")


FAR_FIRST = (4, 3, 5, 2, 6, 1, 7, 0)


def far_first(k):
    return 4 + ((k + 1) // 2) * (1 - 2 * (k % 2))


def place():
    me = lax.axis_index("band")
    return me // 16, (me // 2) % 8, me % 2


def at_place(x, y, c):
    return (x % 8) * 16 + (y % 8) * 2 + c % 2


def signal(sem, peer):
    pl.semaphore_signal(sem, inc=1, device_id={"band": peer}, device_id_type=MESH)


def greet(barrier):
    x, y, c = place()
    for dx in FAR_FIRST:
        for dc in (1, 0):
            if dx or dc:
                signal(barrier, at_place(x + dx, y, c + dc))
    for dy in FAR_FIRST[:7]:
        signal(barrier, at_place(x, y + dy, c))


GREETINGS = 22


def announce(ready):
    x, y, c = place()
    for k, dy in enumerate(FAR_FIRST[:7]):
        signal(ready.at[FAR_FIRST.index((8 - dy) % 8)], at_place(x, y + dy, c))


def exchange(src, dst, send_sem, recv_sem, own_sem, ready=None):
    me = lax.axis_index("band")
    x, y, c = place()
    parts = [((x + dx) % 8) * 16 for dx in FAR_FIRST]
    cores = [(c + 1) % 2, c]

    def send(peer):
        pltpu.make_async_remote_copy(
            src.at[:, peer],
            dst.at[:, me],
            send_sem,
            recv_sem,
            device_id={"band": peer},
            device_id_type=MESH,
        ).start()

    def column(k, carry):
        if ready is not None:
            pl.semaphore_wait(ready.at[k], 1)
        base = ((y + far_first(k)) % 8) * 2
        for part in parts:
            for core in cores:
                send(base + part + core)
        return carry

    lax.fori_loop(0, 7, column, 0)
    for n, part in enumerate(parts):
        for core in cores[: 2 if n < 7 else 1]:
            send(y * 2 + part + core)
    pltpu.make_async_copy(src.at[:, me], dst.at[:, me], own_sem).start()


def wait_exchange(src, dst, send_sem, recv_sem, own_sem, peers):
    me = lax.axis_index("band")
    some = pl.ds(0, peers)
    pltpu.make_async_copy(src.at[:, me], dst.at[:, me], own_sem).wait()
    pltpu.make_async_copy(src.at[:, some], dst.at[:, some], recv_sem).wait()


def wait_sent(src, dst, send_sem, peers):
    some = pl.ds(0, peers)
    pltpu.make_async_copy(src.at[:, some], dst.at[:, some], send_sem).wait()


def main_kernel(
    grid_hbm,
    leg_hbm,
    gw_hbm,
    vm_hbm,
    cp_hbm,
    mr_hbm,
    ll_hbm,
    lo_hbm,
    wn_hbm,
    a_ref,
    t_ref,
    gbuf,
    leg_v,
    gw_v,
    vm_v,
    cp_v,
    mr_v,
    ll_v,
    lo_v,
    wn_v,
    ll_s,
    lo_s,
    wn_s,
    base_c,
    base_s,
    turn_c,
    turn_s,
    facc,
    send1,
    recv1,
    send2,
    recv2,
    lhs,
    l2t,
    inv,
    kmix,
    vz,
    cz,
    rz,
    vpad,
    gpad,
    wall,
    pf,
    zf,
    solved,
    loc_sem,
    grid_sem,
    send_sem,
    recv_sem,
    own_sem,
    ready,
):
    band = lax.axis_index("band")
    fields, width = gbuf.shape
    levels = vm_v.shape[0]
    blocks = width // LANES
    lats = lo_v.shape[1]
    half, rows = leg_v.shape[1:]
    peers = lats - 1
    pairs = 2 * lats
    tiles = send1.shape[0]
    s1 = send1.reshape(tiles, pairs, LANES)
    r1 = recv1.reshape(tiles, pairs, LANES)
    s2 = send2.reshape(tiles, pairs, LANES)
    r2 = recv2.reshape(tiles, pairs, LANES)

    barrier = pltpu.get_barrier_semaphore()
    greet(barrier)
    small = [
        (lo_hbm, lo_s),
        (ll_hbm, ll_s),
        (wn_hbm, wn_v),
        (wn_hbm, wn_s),
        (lo_hbm, lo_v),
        (ll_hbm, ll_v),
        (gw_hbm, gw_v),
        (mr_hbm, mr_v),
        (vm_hbm, vm_v),
        (cp_hbm, cp_v),
        (leg_hbm, leg_v),
    ]
    small = [pltpu.make_async_copy(s, d, loc_sem.at[k]) for k, (s, d) in enumerate(small)]
    for copy in small[:3]:
        copy.start()
    chunks = [(k, min(4, blocks - k)) for k in range(0, blocks, 4)]
    loads = []
    for n, (k, count) in enumerate(chunks):
        part = pl.ds(k * LANES, count * LANES)
        loads.append(pltpu.make_async_copy(grid_hbm.at[:, part], gbuf.at[:, part], grid_sem.at[n]))
        loads[-1].start()
    for copy in small[3:]:
        copy.start()

    facc[fields:, :] = jnp.zeros((facc.shape[0] - fields, pairs), F32)

    for copy in small[:3]:
        copy.wait()
    length = ll_s[0, lo_s[0, band]]
    lane = iota((8, LANES), 1)
    waves8 = jnp.broadcast_to(wn_v[...], (8, LANES))
    waves = jnp.concatenate(
        [take_lanes(waves8, lane // 2 + k * (LANES // 2)) for k in range(2)], axis=1
    )[0:1].astype(F32)
    quarter = (iota((1, pairs), 1) % 2).astype(F32) * 0.25
    length_row = jnp.full((1, pairs), length.astype(F32))
    inv_length = 1.0 / length_row

    def turns(count, stride):
        x = (iota((count, pairs), 0) * stride).astype(F32) * waves
        return (x - jnp.floor(x * inv_length) * length_row) * inv_length

    fine = turns(8, 1) + quarter
    fine_c, fine_s = cos_turn(fine), cos_turn(fine - 0.25)
    mid = turns(16, 8)
    mid_c, mid_s = cos_turn(mid), cos_turn(mid - 0.25)
    for k in range(16):
        c, s = mid_c[k : k + 1], mid_s[k : k + 1]
        base_c[8 * k : 8 * k + 8, :] = c * fine_c - s * fine_s
        base_s[8 * k : 8 * k + 8, :] = s * fine_c + c * fine_s
    far = turns(turn_c.shape[0], LANES)
    turn_c[...] = cos_turn(far)
    turn_s[...] = cos_turn(far - 0.25)
    within = iota((LANES, pairs), 0)
    acc = None
    for n, (k, count) in enumerate(chunks):
        for a in range(k, k + count):
            block = turn_c[a : a + 1, :] * base_c[...] - turn_s[a : a + 1, :] * base_s[...]
            block = jnp.where(within < length - a * LANES, block, 0.0)
            t_ref[a * LANES : (a + 1) * LANES, :] = block.astype(BF16)
        loads[n].wait()
        part = pl.ds(k * LANES, count * LANES)
        product = dot(gbuf[:, part], t_ref[part, :])
        acc = product if acc is None else acc + product
    scale = jnp.where(2.0 * waves < length_row, inv_length, 0.0)
    facc[:fields, :] = acc * scale
    for t in range(tiles):
        s1[t] = facc[t * LANES : (t + 1) * LANES, :].T.astype(BF16)

    pl.semaphore_wait(barrier, GREETINGS)
    announce(ready)
    exchange(send1, recv1, send_sem.at[0], recv_sem.at[0], own_sem.at[0], ready)

    for copy in small[3:]:
        copy.wait()
    wave = wn_s[0, band]
    lat = lo_v[...]
    north = lat < half
    lat_row = jnp.where(north, lat, lats - 1 - lat)
    select = jnp.where(iota((half, lats), 0) == lat_row, 1.0, 0.0)
    sign = jnp.where(north, 1.0, -1.0)
    weight = dot(jnp.broadcast_to(gw_v[...], (8, half)), select, precision=HIGHEST)[0:1]
    select = select.astype(BF16)
    lat8 = jnp.broadcast_to(lat, (8, lats))
    length8 = take_lanes(jnp.broadcast_to(ll_v[...], (8, lats)), lat8)
    length_col = jnp.broadcast_to(length8[0:1].astype(F32), (lats, lats)).T
    lat_col = jnp.broadcast_to(lat.astype(F32), (lats, lats)).T
    north_col = lat_col < half
    sign_col = jnp.where(north_col, 1.0, -1.0)[:, 0:1]
    place_col = jnp.where(north_col, lat_col, lats - 1.0 - lat_col)[:, :half]
    select_t = jnp.where(iota((lats, half), 1).astype(F32) == place_col, 1.0, 0.0).astype(BF16)
    doubling = jnp.where(jnp.full((lats, lats), wave) == 0, 1.0, 2.0)
    wave_f = jnp.full((lats, lats), wave).astype(F32)
    keep_col = jnp.where(2.0 * wave_f < length_col, doubling, 0.0)[:, 0:1]

    rz[...] = jnp.zeros(rz.shape, F32)
    rz[0:1, :levels] = mr_v[...]
    rates = rz[0:1, :]
    for p in range(2):
        table = leg_v[p]
        span = slice(p * rows, (p + 1) * rows)
        degree = iota((rows, LANES), 0) * 2 + (wave + p)
        energy = (degree * (degree + 1)).astype(F32) * (STEP / float(TRUNC * (TRUNC + 1)))
        gain = weight if p == 0 else weight * sign
        own = jnp.where(degree <= TRUNC, dot(table, select, ((0,), (0,))) * gain, 0.0)
        lhs[span, :LANES] = own.astype(BF16)
        lhs[span, LANES:] = (own * -energy).astype(BF16)
        for t in range(2):
            inv[span, t * LANES : (t + 1) * LANES] = 1.0 / (
                1.0 + energy * rates[:, t * LANES : (t + 1) * LANES]
            )
        gain_col = keep_col if p == 0 else keep_col * sign_col
        l2t[:, span] = (dot(select_t, table) * gain_col).astype(BF16)
    mix = dot(l2t[...], lhs[:, :LANES]).astype(BF16)
    spread = []
    for q in range(2):
        each = jnp.where(iota((pairs, lats), 0) == iota((pairs, lats), 1) * 2 + q, 1.0, 0.0)
        each = each.astype(BF16)
        spread.append(dot(dot(each, mix).astype(BF16), each, ((1,), (1,))))
    kmix[...] = (spread[0] + spread[1]).astype(BF16)

    vz[...] = jnp.zeros(vz.shape, F32)
    cz[...] = jnp.zeros(cz.shape, F32)
    vz[:levels, :levels] = vm_v[...]
    cz[:levels, :levels] = cp_v[...]
    modes, couple = vz[...], cz[...]
    square = modes.shape
    vpad[...] = modes.astype(BF16)
    gap = levels - LANES
    shift = jnp.where(iota(square, 0) == iota(square, 1) + gap, 1.0, 0.0)
    moved = dot(shift, couple, ((1,), (1,)), precision=HIGHEST)
    gpad[...] = dot(moved, modes, precision=HIGHEST).astype(BF16)
    wide = (square[0], tiles * LANES)
    shift = jnp.where(iota(wide, 1) == iota(wide, 0) + levels, 1.0, 0.0)
    same = jnp.where(iota(wide, 1) == iota(wide, 0), 1.0, 0.0)
    spread_out = same - STEP * dot(couple, shift, ((0,), (0,)), precision=HIGHEST)
    wall[...] = dot(modes, spread_out, ((0,), (0,)), precision=HIGHEST).astype(BF16)

    wait_exchange(send1, recv1, send_sem.at[0], recv_sem.at[0], own_sem.at[0], peers)
    f0, f1, f2 = r1[0], r1[1], r1[2]
    last = jnp.concatenate([f1, f2], axis=1)
    in_d = dot(jnp.concatenate([f0, f1], axis=1), vpad[...])
    in_p = dot(last, gpad[...])
    for t in range(2):
        pf[t] = in_d[:, t * LANES : (t + 1) * LANES]
        pf[2 + t] = in_p[:, t * LANES : (t + 1) * LANES]

    parts = [pl.ds(q, lats, stride=2) for q in range(2)]
    rhs = []
    for part in parts:
        both = [jnp.concatenate([pf[n, part, :], pf[n + 1, part, :]], axis=1) for n in (0, 2)]
        rhs.append(jnp.concatenate(both, axis=0).astype(BF16))

    wide_rhs = jnp.concatenate(rhs, axis=1)
    own_p = dot(kmix[...], last)
    for k in range(0, 2 * rows, 256):
        span = slice(k, k + 256)
        each = dot(lhs[span, :], wide_rhs)
        share = inv[span, :]
        for q in range(2):
            half_q = slice(2 * q * LANES, 2 * (q + 1) * LANES)
            solved[span, half_q] = (each[:, half_q] * share).astype(BF16)
    both = dot(l2t[...], solved[...])
    totals = [both[:, : 2 * LANES], both[:, 2 * LANES :]]
    for q, part in enumerate(parts):
        for t in range(2):
            zf[t, part, :] = totals[q][:, t * LANES : (t + 1) * LANES]

    back = jnp.concatenate([zf[0], zf[1]], axis=1).astype(BF16)
    out = dot(back, wall[...])
    only_p = iota((pairs, LANES), 1) >= gap
    s2[0] = out[:, :LANES].astype(BF16)
    s2[1] = (out[:, LANES : 2 * LANES] + jnp.where(only_p, own_p[:, :LANES], 0.0)).astype(BF16)
    s2[2] = (out[:, 2 * LANES :] + own_p[:, LANES:]).astype(BF16)

    exchange(send2, recv2, send_sem.at[1], recv_sem.at[1], own_sem.at[1])
    wait_sent(send1, recv1, send_sem.at[0], peers)
    wait_exchange(send2, recv2, send_sem.at[1], recv_sem.at[1], own_sem.at[1], peers)
    for t in range(tiles):
        a_ref[t * LANES : (t + 1) * LANES, :] = r2[t].astype(F32).T.astype(BF16)
    wait_sent(send2, recv2, send_sem.at[1], peers)


def inverse_kernel(a_ref, t_ref, out_hbm, obuf, sem):
    fields, width = obuf.shape
    step = 4 * LANES
    copies = []
    for n, k in enumerate(range(0, width, step)):
        part = pl.ds(k, min(step, width - k))
        obuf[:, part] = dot(a_ref[:fields, :], t_ref[part, :], ((1,), (1,))).astype(BF16)
        copies.append(pltpu.make_async_copy(obuf.at[:, part], out_hbm.at[:, part], sem.at[n]))
        copies[-1].start()
    for copy in copies:
        copy.wait()


def per_device(grid_in, legendre, gauss_weight, vertical_modes, coupling, mode_rates, loop_length, lat_order, wave_number):
    fields, width = grid_in.shape[1:]
    rows, half = legendre.shape[2:]
    levels = vertical_modes.shape[0]
    lats = lat_order.shape[0]
    pairs = 2 * lats
    tiles = -(-fields // LANES)
    blocks = width // LANES
    operands = [
        grid_in.reshape(fields, width),
        jnp.swapaxes(legendre.reshape(2, rows, half), 1, 2),
        gauss_weight.reshape(1, half),
        vertical_modes,
        coupling,
        mode_rates.reshape(1, levels),
        loop_length.reshape(1, lats),
        lat_order.reshape(1, lats),
        wave_number.reshape(1, lats),
    ]
    hbm = pl.BlockSpec(memory_space=pltpu.HBM)
    vmem = pl.BlockSpec(memory_space=pltpu.VMEM)
    dma = pltpu.SemaphoreType.DMA
    a_mat, table = pl.pallas_call(
        main_kernel,
        out_shape=(
            pltpu.VMEM((tiles * LANES, pairs), BF16),
            pltpu.VMEM((width, pairs), BF16),
        ),
        in_specs=[hbm] * 9,
        out_specs=(vmem, vmem),
        scratch_shapes=[
            pltpu.VMEM((fields, width), BF16),
            pltpu.VMEM((2, half, rows), BF16),
            pltpu.VMEM((1, half), F32),
            pltpu.VMEM((levels, levels), F32),
            pltpu.VMEM((levels, levels), F32),
            pltpu.VMEM((1, levels), F32),
            pltpu.VMEM((1, lats), I32),
            pltpu.VMEM((1, lats), I32),
            pltpu.VMEM((1, lats), I32),
            pltpu.SMEM((1, lats), I32),
            pltpu.SMEM((1, lats), I32),
            pltpu.SMEM((1, lats), I32),
            pltpu.VMEM((LANES, pairs), F32),
            pltpu.VMEM((LANES, pairs), F32),
            pltpu.VMEM((-(-blocks // 8) * 8, pairs), F32),
            pltpu.VMEM((-(-blocks // 8) * 8, pairs), F32),
            pltpu.VMEM((tiles * LANES, pairs), F32),
            pltpu.VMEM((tiles, lats, 2, LANES), BF16),
            pltpu.VMEM((tiles, lats, 2, LANES), BF16),
            pltpu.VMEM((tiles, lats, 2, LANES), BF16),
            pltpu.VMEM((tiles, lats, 2, LANES), BF16),
            pltpu.VMEM((2 * rows, 2 * LANES), BF16),
            pltpu.VMEM((lats, 2 * rows), BF16),
            pltpu.VMEM((2 * rows, 2 * LANES), F32),
            pltpu.VMEM((pairs, pairs), BF16),
            pltpu.VMEM((2 * LANES, 2 * LANES), F32),
            pltpu.VMEM((2 * LANES, 2 * LANES), F32),
            pltpu.VMEM((8, 2 * LANES), F32),
            pltpu.VMEM((2 * LANES, 2 * LANES), BF16),
            pltpu.VMEM((2 * LANES, 2 * LANES), BF16),
            pltpu.VMEM((2 * LANES, tiles * LANES), BF16),
            pltpu.VMEM((4, pairs, LANES), F32),
            pltpu.VMEM((2, pairs, LANES), F32),
            pltpu.VMEM((2 * rows, 4 * LANES), BF16),
            dma((11,)),
            dma((-(-blocks // 4),)),
            dma((2,)),
            dma((2,)),
            dma((2,)),
            pltpu.SemaphoreType.REGULAR((7,)),
        ],
        compiler_params=pltpu.CompilerParams(
            collective_id=1, has_side_effects=True, vmem_limit_bytes=40 * 2**20
        ),
        name="spectral_step",
    )(*[pltpu.with_memory_space_constraint(each, pltpu.HBM) for each in operands])
    a_mat = pltpu.with_memory_space_constraint(a_mat, pltpu.VMEM)
    table = pltpu.with_memory_space_constraint(table, pltpu.VMEM)
    points = pl.pallas_call(
        inverse_kernel,
        out_shape=jax.ShapeDtypeStruct((fields, width), BF16),
        in_specs=[vmem, vmem],
        out_specs=hbm,
        scratch_shapes=[pltpu.VMEM((fields, width), BF16), dma((-(-blocks // 4),))],
        compiler_params=pltpu.CompilerParams(vmem_limit_bytes=16 * 2**20),
        name="inverse_loop",
    )(a_mat, table)
    return points.reshape(grid_in.shape)


def solution(mesh):
    whole = P(("member", "band"), None, None)
    in_specs = (whole, P("band", None, None, None)) + (P(),) * 7
    return jax.shard_map(per_device, mesh=mesh, in_specs=in_specs, out_specs=whole, check_vma=False)
```

```python
import functools
import math

import jax
import jax.numpy as jnp
from jax import lax
from jax.experimental import pallas as pl
from jax.experimental.pallas import tpu as pltpu
from jax.sharding import PartitionSpec as P

TRUNC = 1279
STEP = 0.5
LANES = 128
MESH = pl.DeviceIdType.MESH
HIGHEST = lax.Precision.HIGHEST
F32 = jnp.float32
BF16 = jnp.bfloat16
I32 = jnp.int32

SIN_TERMS = [
    (-1.0) ** k * (2.0 * math.pi) ** (2 * k + 1) / math.factorial(2 * k + 1) for k in range(6)
]


def cos_turn(turn):
    near = turn - jnp.floor(turn + 0.5)
    z = 0.25 - jnp.abs(near)
    z2 = z * z
    total = jnp.full_like(z, SIN_TERMS[-1])
    for term in SIN_TERMS[-2::-1]:
        total = total * z2 + term
    return total * z


def iota(shape, dim):
    return lax.broadcasted_iota(I32, shape, dim)


def dot(a, b, dims=((1,), (0,)), precision=None):
    return lax.dot_general(a, b, (dims, ((), ())), precision=precision, preferred_element_type=F32)


def take_lanes(row8, index):
    return jnp.take_along_axis(row8, index, axis=1, mode="promise_in_bounds")


FAR_FIRST = (4, 3, 5, 2, 6, 1, 7, 0)


def far_first(k):
    return 4 + ((k + 1) // 2) * (1 - 2 * (k % 2))


def place():
    me = lax.axis_index("band")
    return me // 16, (me // 2) % 8, me % 2


def at_place(x, y, c):
    return (x % 8) * 16 + (y % 8) * 2 + c % 2


def signal(sem, peer):
    pl.semaphore_signal(sem, inc=1, device_id={"band": peer}, device_id_type=MESH)


def greet(barrier):
    x, y, c = place()
    for dy in FAR_FIRST:
        for dc in (1, 0):
            if dy or dc:
                signal(barrier, at_place(x, y + dy, c + dc))
    for dx in FAR_FIRST[:7]:
        signal(barrier, at_place(x + dx, y, c))


GREETINGS = 22


def announce(ready):
    x, y, c = place()
    for dx in FAR_FIRST[:7]:
        signal(ready.at[FAR_FIRST.index((8 - dx) % 8)], at_place(x + dx, y, c))


def exchange(src, dst, send_sem, recv_sem, own_sem, ready=None):
    me = lax.axis_index("band")
    x, y, c = place()
    outer, inner = ((x, 16), (y, 2)) if ready is not None else ((y, 2), (x, 16))
    parts = [((inner[0] + d) % 8) * inner[1] for d in FAR_FIRST]
    cores = [(c + 1) % 2, c]

    def send(peer):
        pltpu.make_async_remote_copy(
            src.at[:, peer],
            dst.at[:, me],
            send_sem,
            recv_sem,
            device_id={"band": peer},
            device_id_type=MESH,
        ).start()

    def line(k, carry):
        if ready is not None:
            pl.semaphore_wait(ready.at[k], 1)
        base = ((outer[0] + far_first(k)) % 8) * outer[1]
        for part in parts:
            for core in cores:
                send(base + part + core)
        return carry

    lax.fori_loop(0, 7, line, 0)
    for n, part in enumerate(parts):
        for core in cores[: 2 if n < 7 else 1]:
            send(outer[0] * outer[1] + part + core)
    pltpu.make_async_copy(src.at[:, me], dst.at[:, me], own_sem).start()


def wait_exchange(src, dst, send_sem, recv_sem, own_sem, peers):
    me = lax.axis_index("band")
    some = pl.ds(0, peers)
    pltpu.make_async_copy(src.at[:, me], dst.at[:, me], own_sem).wait()
    pltpu.make_async_copy(src.at[:, some], dst.at[:, some], recv_sem).wait()


def wait_sent(src, dst, send_sem, peers):
    some = pl.ds(0, peers)
    pltpu.make_async_copy(src.at[:, some], dst.at[:, some], send_sem).wait()


def main_kernel(
    grid_hbm,
    leg_hbm,
    gw_hbm,
    vm_hbm,
    cp_hbm,
    mr_hbm,
    ll_hbm,
    lo_hbm,
    wn_hbm,
    a_ref,
    t_ref,
    gbuf,
    leg_v,
    gw_v,
    vm_v,
    cp_v,
    mr_v,
    ll_v,
    lo_v,
    wn_v,
    ll_s,
    lo_s,
    wn_s,
    base_c,
    base_s,
    turn_c,
    turn_s,
    facc,
    send1,
    recv1,
    send2,
    recv2,
    lhs,
    l2t,
    inv,
    kmix,
    vz,
    cz,
    rz,
    vpad,
    gpad,
    wall,
    pf,
    zf,
    solved,
    loc_sem,
    grid_sem,
    send_sem,
    recv_sem,
    own_sem,
    ready,
):
    band = lax.axis_index("band")
    fields, width = gbuf.shape
    levels = vm_v.shape[0]
    blocks = width // LANES
    lats = lo_v.shape[1]
    half, rows = leg_v.shape[1:]
    peers = lats - 1
    pairs = 2 * lats
    tiles = send1.shape[0]
    s1 = send1.reshape(tiles, pairs, LANES)
    r1 = recv1.reshape(tiles, pairs, LANES)
    s2 = send2.reshape(tiles, pairs, LANES)
    r2 = recv2.reshape(tiles, pairs, LANES)

    barrier = pltpu.get_barrier_semaphore()
    greet(barrier)
    small = [
        (lo_hbm, lo_s),
        (ll_hbm, ll_s),
        (wn_hbm, wn_v),
        (wn_hbm, wn_s),
        (lo_hbm, lo_v),
        (ll_hbm, ll_v),
        (gw_hbm, gw_v),
        (mr_hbm, mr_v),
        (vm_hbm, vm_v),
        (cp_hbm, cp_v),
        (leg_hbm, leg_v),
    ]
    small = [pltpu.make_async_copy(s, d, loc_sem.at[k]) for k, (s, d) in enumerate(small)]
    for copy in small[:3]:
        copy.start()
    chunks = [(k, min(4, blocks - k)) for k in range(0, blocks, 4)]
    loads = []
    for n, (k, count) in enumerate(chunks):
        part = pl.ds(k * LANES, count * LANES)
        loads.append(pltpu.make_async_copy(grid_hbm.at[:, part], gbuf.at[:, part], grid_sem.at[n]))
        loads[-1].start()
    for copy in small[3:]:
        copy.start()

    facc[fields:, :] = jnp.zeros((facc.shape[0] - fields, pairs), F32)

    for copy in small[:3]:
        copy.wait()
    length = ll_s[0, lo_s[0, band]]
    lane = iota((8, LANES), 1)
    waves8 = jnp.broadcast_to(wn_v[...], (8, LANES))
    waves = jnp.concatenate(
        [take_lanes(waves8, lane // 2 + k * (LANES // 2)) for k in range(2)], axis=1
    )[0:1].astype(F32)
    quarter = (iota((1, pairs), 1) % 2).astype(F32) * 0.25
    length_row = jnp.full((1, pairs), length.astype(F32))
    inv_length = 1.0 / length_row

    def turns(count, stride):
        x = (iota((count, pairs), 0) * stride).astype(F32) * waves
        return (x - jnp.floor(x * inv_length) * length_row) * inv_length

    fine = turns(8, 1) + quarter
    fine_c, fine_s = cos_turn(fine), cos_turn(fine - 0.25)
    mid = turns(16, 8)
    mid_c, mid_s = cos_turn(mid), cos_turn(mid - 0.25)
    for k in range(16):
        c, s = mid_c[k : k + 1], mid_s[k : k + 1]
        base_c[8 * k : 8 * k + 8, :] = c * fine_c - s * fine_s
        base_s[8 * k : 8 * k + 8, :] = s * fine_c + c * fine_s
    far = turns(turn_c.shape[0], LANES)
    turn_c[...] = cos_turn(far)
    turn_s[...] = cos_turn(far - 0.25)
    group = 16
    within = iota((group, pairs), 0)
    middle = -(-fields // 32) * 16
    split = [slice(0, middle), slice(middle, fields)]
    acc = [None, None]
    for n, (k, count) in enumerate(chunks):
        for g in range(0, LANES, group):
            base = base_c[g : g + group, :], base_s[g : g + group, :]
            for a in range(k, k + count):
                block = turn_c[a : a + 1, :] * base[0] - turn_s[a : a + 1, :] * base[1]
                block = jnp.where(within < length - (a * LANES + g), block, 0.0)
                t_ref[a * LANES + g : a * LANES + g + group, :] = block.astype(BF16)
        loads[n].wait()
        part = pl.ds(k * LANES, count * LANES)
        for m, some in enumerate(split):
            product = dot(gbuf[some, part], t_ref[part, :])
            acc[m] = product if n == 0 else acc[m] + product
        if n == len(chunks) // 2 - 1:
            pl.semaphore_wait(barrier, GREETINGS)
            announce(ready)
    scale = jnp.where(2.0 * waves < length_row, inv_length, 0.0)
    for some, total in zip(split, acc):
        facc[some, :] = total * scale
    for t in range(tiles):
        s1[t] = facc[t * LANES : (t + 1) * LANES, :].T.astype(BF16)

    exchange(send1, recv1, send_sem.at[0], recv_sem.at[0], own_sem.at[0], ready)

    for copy in small[3:]:
        copy.wait()
    wave = wn_s[0, band]
    lat = lo_v[...]
    north = lat < half
    lat_row = jnp.where(north, lat, lats - 1 - lat)
    select = jnp.where(iota((half, lats), 0) == lat_row, 1.0, 0.0)
    sign = jnp.where(north, 1.0, -1.0)
    weight = dot(jnp.broadcast_to(gw_v[...], (8, half)), select, precision=HIGHEST)[0:1]
    select = select.astype(BF16)
    lat8 = jnp.broadcast_to(lat, (8, lats))
    length8 = take_lanes(jnp.broadcast_to(ll_v[...], (8, lats)), lat8)
    length_col = jnp.broadcast_to(length8[0:1].astype(F32), (lats, lats)).T
    lat_col = jnp.broadcast_to(lat.astype(F32), (lats, lats)).T
    north_col = lat_col < half
    sign_col = jnp.where(north_col, 1.0, -1.0)[:, 0:1]
    place_col = jnp.where(north_col, lat_col, lats - 1.0 - lat_col)[:, :half]
    select_t = jnp.where(iota((lats, half), 1).astype(F32) == place_col, 1.0, 0.0).astype(BF16)
    doubling = jnp.where(jnp.full((lats, lats), wave) == 0, 1.0, 2.0)
    wave_f = jnp.full((lats, lats), wave).astype(F32)
    keep_col = jnp.where(2.0 * wave_f < length_col, doubling, 0.0)[:, 0:1]

    rz[...] = jnp.zeros(rz.shape, F32)
    rz[0:1, :levels] = mr_v[...]
    rates = rz[0:1, :]
    for p in range(2):
        table = leg_v[p]
        span = slice(p * rows, (p + 1) * rows)
        degree = iota((rows, LANES), 0) * 2 + (wave + p)
        energy = (degree * (degree + 1)).astype(F32) * (STEP / float(TRUNC * (TRUNC + 1)))
        gain = weight if p == 0 else weight * sign
        own = jnp.where(degree <= TRUNC, dot(table, select, ((0,), (0,))) * gain, 0.0)
        lhs[span, :LANES] = own.astype(BF16)
        lhs[span, LANES:] = (own * -energy).astype(BF16)
        for t in range(2):
            inv[span, t * LANES : (t + 1) * LANES] = 1.0 / (
                1.0 + energy * rates[:, t * LANES : (t + 1) * LANES]
            )
        gain_col = keep_col if p == 0 else keep_col * sign_col
        l2t[:, span] = (dot(select_t, table) * gain_col).astype(BF16)
    mix = dot(l2t[...], lhs[:, :LANES]).astype(BF16)
    spread = []
    for q in range(2):
        each = jnp.where(iota((pairs, lats), 0) == iota((pairs, lats), 1) * 2 + q, 1.0, 0.0)
        each = each.astype(BF16)
        spread.append(dot(dot(each, mix).astype(BF16), each, ((1,), (1,))))
    kmix[...] = (spread[0] + spread[1]).astype(BF16)

    vz[...] = jnp.zeros(vz.shape, F32)
    cz[...] = jnp.zeros(cz.shape, F32)
    vz[:levels, :levels] = vm_v[...]
    cz[:levels, :levels] = cp_v[...]
    modes, couple = vz[...], cz[...]
    square = modes.shape
    vpad[...] = modes.astype(BF16)
    gap = levels - LANES
    shift = jnp.where(iota(square, 0) == iota(square, 1) + gap, 1.0, 0.0)
    moved = dot(shift, couple, ((1,), (1,)), precision=HIGHEST)
    gpad[...] = dot(moved, modes, precision=HIGHEST).astype(BF16)
    wide = (square[0], tiles * LANES)
    shift = jnp.where(iota(wide, 1) == iota(wide, 0) + levels, 1.0, 0.0)
    same = jnp.where(iota(wide, 1) == iota(wide, 0), 1.0, 0.0)
    spread_out = same - STEP * dot(couple, shift, ((0,), (0,)), precision=HIGHEST)
    wall[...] = dot(modes, spread_out, ((0,), (0,)), precision=HIGHEST).astype(BF16)

    wait_exchange(send1, recv1, send_sem.at[0], recv_sem.at[0], own_sem.at[0], peers)
    f0, f1, f2 = r1[0], r1[1], r1[2]
    last = jnp.concatenate([f1, f2], axis=1)
    in_d = dot(jnp.concatenate([f0, f1], axis=1), vpad[...])
    in_p = dot(last, gpad[...])
    for t in range(2):
        pf[t] = in_d[:, t * LANES : (t + 1) * LANES]
        pf[2 + t] = in_p[:, t * LANES : (t + 1) * LANES]

    parts = [pl.ds(q, lats, stride=2) for q in range(2)]
    rhs = []
    for part in parts:
        both = [jnp.concatenate([pf[n, part, :], pf[n + 1, part, :]], axis=1) for n in (0, 2)]
        rhs.append(jnp.concatenate(both, axis=0).astype(BF16))

    wide_rhs = jnp.concatenate(rhs, axis=1)
    own_p = dot(kmix[...], last)
    for k in range(0, 2 * rows, 256):
        span = slice(k, k + 256)
        each = dot(lhs[span, :], wide_rhs)
        share = inv[span, :]
        for q in range(2):
            half_q = slice(2 * q * LANES, 2 * (q + 1) * LANES)
            solved[span, half_q] = (each[:, half_q] * share).astype(BF16)
    both = dot(l2t[...], solved[...])
    totals = [both[:, : 2 * LANES], both[:, 2 * LANES :]]
    for q, part in enumerate(parts):
        for t in range(2):
            zf[t, part, :] = totals[q][:, t * LANES : (t + 1) * LANES]

    back = jnp.concatenate([zf[0], zf[1]], axis=1).astype(BF16)
    out = dot(back, wall[...])
    only_p = iota((pairs, LANES), 1) >= gap
    s2[0] = out[:, :LANES].astype(BF16)
    s2[1] = (out[:, LANES : 2 * LANES] + jnp.where(only_p, own_p[:, :LANES], 0.0)).astype(BF16)
    s2[2] = (out[:, 2 * LANES :] + own_p[:, LANES:]).astype(BF16)

    exchange(send2, recv2, send_sem.at[1], recv_sem.at[1], own_sem.at[1])
    wait_sent(send1, recv1, send_sem.at[0], peers)
    wait_exchange(send2, recv2, send_sem.at[1], recv_sem.at[1], own_sem.at[1], peers)
    for t in range(tiles):
        a_ref[t * LANES : (t + 1) * LANES, :] = r2[t].astype(F32).T.astype(BF16)
    wait_sent(send2, recv2, send_sem.at[1], peers)


def inverse_kernel(a_ref, t_ref, out_hbm, obuf, sem):
    fields, width = obuf.shape
    step = 4 * LANES
    copies = []
    for n, k in enumerate(range(0, width, step)):
        part = pl.ds(k, min(step, width - k))
        obuf[:, part] = dot(a_ref[:fields, :], t_ref[part, :], ((1,), (1,))).astype(BF16)
        copies.append(pltpu.make_async_copy(obuf.at[:, part], out_hbm.at[:, part], sem.at[n]))
        copies[-1].start()
    for copy in copies:
        copy.wait()


def per_device(grid_in, legendre, gauss_weight, vertical_modes, coupling, mode_rates, loop_length, lat_order, wave_number):
    fields, width = grid_in.shape[1:]
    rows, half = legendre.shape[2:]
    levels = vertical_modes.shape[0]
    lats = lat_order.shape[0]
    pairs = 2 * lats
    tiles = -(-fields // LANES)
    blocks = width // LANES
    operands = [
        grid_in.reshape(fields, width),
        jnp.swapaxes(legendre.reshape(2, rows, half), 1, 2),
        gauss_weight.reshape(1, half),
        vertical_modes,
        coupling,
        mode_rates.reshape(1, levels),
        loop_length.reshape(1, lats),
        lat_order.reshape(1, lats),
        wave_number.reshape(1, lats),
    ]
    hbm = pl.BlockSpec(memory_space=pltpu.HBM)
    vmem = pl.BlockSpec(memory_space=pltpu.VMEM)
    dma = pltpu.SemaphoreType.DMA
    a_mat, table = pl.pallas_call(
        main_kernel,
        out_shape=(
            pltpu.VMEM((tiles * LANES, pairs), BF16),
            pltpu.VMEM((width, pairs), BF16),
        ),
        in_specs=[hbm] * 9,
        out_specs=(vmem, vmem),
        scratch_shapes=[
            pltpu.VMEM((fields, width), BF16),
            pltpu.VMEM((2, half, rows), BF16),
            pltpu.VMEM((1, half), F32),
            pltpu.VMEM((levels, levels), F32),
            pltpu.VMEM((levels, levels), F32),
            pltpu.VMEM((1, levels), F32),
            pltpu.VMEM((1, lats), I32),
            pltpu.VMEM((1, lats), I32),
            pltpu.VMEM((1, lats), I32),
            pltpu.SMEM((1, lats), I32),
            pltpu.SMEM((1, lats), I32),
            pltpu.SMEM((1, lats), I32),
            pltpu.VMEM((LANES, pairs), F32),
            pltpu.VMEM((LANES, pairs), F32),
            pltpu.VMEM((-(-blocks // 8) * 8, pairs), F32),
            pltpu.VMEM((-(-blocks // 8) * 8, pairs), F32),
            pltpu.VMEM((tiles * LANES, pairs), F32),
            pltpu.VMEM((tiles, lats, 2, LANES), BF16),
            pltpu.VMEM((tiles, lats, 2, LANES), BF16),
            pltpu.VMEM((tiles, lats, 2, LANES), BF16),
            pltpu.VMEM((tiles, lats, 2, LANES), BF16),
            pltpu.VMEM((2 * rows, 2 * LANES), BF16),
            pltpu.VMEM((lats, 2 * rows), BF16),
            pltpu.VMEM((2 * rows, 2 * LANES), F32),
            pltpu.VMEM((pairs, pairs), BF16),
            pltpu.VMEM((2 * LANES, 2 * LANES), F32),
            pltpu.VMEM((2 * LANES, 2 * LANES), F32),
            pltpu.VMEM((8, 2 * LANES), F32),
            pltpu.VMEM((2 * LANES, 2 * LANES), BF16),
            pltpu.VMEM((2 * LANES, 2 * LANES), BF16),
            pltpu.VMEM((2 * LANES, tiles * LANES), BF16),
            pltpu.VMEM((4, pairs, LANES), F32),
            pltpu.VMEM((2, pairs, LANES), F32),
            pltpu.VMEM((2 * rows, 4 * LANES), BF16),
            dma((11,)),
            dma((-(-blocks // 4),)),
            dma((2,)),
            dma((2,)),
            dma((2,)),
            pltpu.SemaphoreType.REGULAR((7,)),
        ],
        compiler_params=pltpu.CompilerParams(
            collective_id=1, has_side_effects=True, vmem_limit_bytes=40 * 2**20
        ),
        name="spectral_step",
    )(*[pltpu.with_memory_space_constraint(each, pltpu.HBM) for each in operands])
    a_mat = pltpu.with_memory_space_constraint(a_mat, pltpu.VMEM)
    table = pltpu.with_memory_space_constraint(table, pltpu.VMEM)
    points = pl.pallas_call(
        inverse_kernel,
        out_shape=jax.ShapeDtypeStruct((fields, width), BF16),
        in_specs=[vmem, vmem],
        out_specs=hbm,
        scratch_shapes=[pltpu.VMEM((fields, width), BF16), dma((-(-blocks // 4),))],
        compiler_params=pltpu.CompilerParams(vmem_limit_bytes=16 * 2**20),
        name="inverse_loop",
    )(a_mat, table)
    return points.reshape(grid_in.shape)


def solution(mesh):
    whole = P(("member", "band"), None, None)
    in_specs = (whole, P("band", None, None, None)) + (P(),) * 7
    return jax.shard_map(per_device, mesh=mesh, in_specs=in_specs, out_specs=whole, check_vma=False)
```

```python
import functools
import math

import jax
import jax.numpy as jnp
from jax import lax
from jax.experimental import pallas as pl
from jax.experimental.pallas import tpu as pltpu
from jax.sharding import PartitionSpec as P

TRUNC = 1279
STEP = 0.5
LANES = 128
MESH = pl.DeviceIdType.MESH
HIGHEST = lax.Precision.HIGHEST
F32 = jnp.float32
BF16 = jnp.bfloat16
I32 = jnp.int32

SIN_TERMS = [
    (-1.0) ** k * (2.0 * math.pi) ** (2 * k + 1) / math.factorial(2 * k + 1) for k in range(6)
]


def cos_turn(turn):
    near = turn - jnp.floor(turn + 0.5)
    z = 0.25 - jnp.abs(near)
    z2 = z * z
    total = jnp.full_like(z, SIN_TERMS[-1])
    for term in SIN_TERMS[-2::-1]:
        total = total * z2 + term
    return total * z


def iota(shape, dim):
    return lax.broadcasted_iota(I32, shape, dim)


def dot(a, b, dims=((1,), (0,)), precision=None):
    return lax.dot_general(a, b, (dims, ((), ())), precision=precision, preferred_element_type=F32)


def take_lanes(row8, index):
    return jnp.take_along_axis(row8, index, axis=1, mode="promise_in_bounds")


FAR_FIRST = (4, 3, 5, 2, 6, 1, 7, 0)


def far_first(k):
    return 4 + ((k + 1) // 2) * (1 - 2 * (k % 2))


def place():
    me = lax.axis_index("band")
    return me // 16, (me // 2) % 8, me % 2


def at_place(x, y, c):
    return (x % 8) * 16 + (y % 8) * 2 + c % 2


def signal(sem, peer):
    pl.semaphore_signal(sem, inc=1, device_id={"band": peer}, device_id_type=MESH)


def greet(barrier):
    x, y, c = place()
    for dy in FAR_FIRST:
        for dc in (1, 0):
            if dy or dc:
                signal(barrier, at_place(x, y + dy, c + dc))
    for dx in FAR_FIRST[:7]:
        signal(barrier, at_place(x + dx, y, c))


GREETINGS = 22


def announce(ready):
    x, y, c = place()
    for dx in FAR_FIRST[:7]:
        signal(ready.at[FAR_FIRST.index((8 - dx) % 8)], at_place(x + dx, y, c))


def exchange(src, dst, send_sem, recv_sem, own_sem, ready=None):
    me = lax.axis_index("band")
    x, y, c = place()
    outer, inner = ((x, 16), (y, 2)) if ready is not None else ((y, 2), (x, 16))
    parts = [((inner[0] + d) % 8) * inner[1] for d in FAR_FIRST]
    cores = [(c + 1) % 2, c]

    def send(peer):
        pltpu.make_async_remote_copy(
            src.at[:, peer],
            dst.at[:, me],
            send_sem,
            recv_sem,
            device_id={"band": peer},
            device_id_type=MESH,
        ).start()

    def line(k, carry):
        if ready is not None:
            pl.semaphore_wait(ready.at[k], 1)
        base = ((outer[0] + far_first(k)) % 8) * outer[1]
        for part in parts:
            for core in cores:
                send(base + part + core)
        return carry

    def own_line():
        for n, part in enumerate(parts):
            for core in cores[: 2 if n < 7 else 1]:
                send(outer[0] * outer[1] + part + core)

    if ready is not None:
        own_line()
    lax.fori_loop(0, 7, line, 0)
    if ready is None:
        own_line()
    pltpu.make_async_copy(src.at[:, me], dst.at[:, me], own_sem).start()


def wait_exchange(src, dst, send_sem, recv_sem, own_sem, peers):
    me = lax.axis_index("band")
    some = pl.ds(0, peers)
    pltpu.make_async_copy(src.at[:, me], dst.at[:, me], own_sem).wait()
    pltpu.make_async_copy(src.at[:, some], dst.at[:, some], recv_sem).wait()


def wait_sent(src, dst, send_sem, peers):
    some = pl.ds(0, peers)
    pltpu.make_async_copy(src.at[:, some], dst.at[:, some], send_sem).wait()


def main_kernel(
    grid_hbm,
    leg_hbm,
    gw_hbm,
    vm_hbm,
    cp_hbm,
    mr_hbm,
    ll_hbm,
    lo_hbm,
    wn_hbm,
    a_ref,
    t_ref,
    gbuf,
    leg_v,
    gw_v,
    vm_v,
    cp_v,
    mr_v,
    ll_v,
    lo_v,
    wn_v,
    ll_s,
    lo_s,
    wn_s,
    base_c,
    base_s,
    turn_c,
    turn_s,
    facc,
    send1,
    recv1,
    send2,
    recv2,
    lhs,
    l2t,
    inv,
    kmix,
    vz,
    cz,
    rz,
    vpad,
    gpad,
    wall,
    pf,
    zf,
    solved,
    loc_sem,
    grid_sem,
    send_sem,
    recv_sem,
    own_sem,
    ready,
):
    band = lax.axis_index("band")
    fields, width = gbuf.shape
    levels = vm_v.shape[0]
    blocks = width // LANES
    lats = lo_v.shape[1]
    half, rows = leg_v.shape[1:]
    peers = lats - 1
    pairs = 2 * lats
    tiles = send1.shape[0]
    s1 = send1.reshape(tiles, pairs, LANES)
    r1 = recv1.reshape(tiles, pairs, LANES)
    s2 = send2.reshape(tiles, pairs, LANES)
    r2 = recv2.reshape(tiles, pairs, LANES)

    barrier = pltpu.get_barrier_semaphore()
    greet(barrier)
    small = [
        (lo_hbm, lo_s),
        (ll_hbm, ll_s),
        (wn_hbm, wn_v),
        (wn_hbm, wn_s),
        (lo_hbm, lo_v),
        (ll_hbm, ll_v),
        (gw_hbm, gw_v),
        (mr_hbm, mr_v),
        (vm_hbm, vm_v),
        (cp_hbm, cp_v),
        (leg_hbm, leg_v),
    ]
    small = [pltpu.make_async_copy(s, d, loc_sem.at[k]) for k, (s, d) in enumerate(small)]
    for copy in small[:3]:
        copy.start()
    chunks = [(k, min(4, blocks - k)) for k in range(0, blocks, 4)]
    loads = []
    for n, (k, count) in enumerate(chunks):
        part = pl.ds(k * LANES, count * LANES)
        loads.append(pltpu.make_async_copy(grid_hbm.at[:, part], gbuf.at[:, part], grid_sem.at[n]))
        loads[-1].start()
    for copy in small[3:]:
        copy.start()

    facc[fields:, :] = jnp.zeros((facc.shape[0] - fields, pairs), F32)

    for copy in small[:3]:
        copy.wait()
    length = ll_s[0, lo_s[0, band]]
    lane = iota((8, LANES), 1)
    waves8 = jnp.broadcast_to(wn_v[...], (8, LANES))
    waves = jnp.concatenate(
        [take_lanes(waves8, lane // 2 + k * (LANES // 2)) for k in range(2)], axis=1
    )[0:1].astype(F32)
    quarter = (iota((1, pairs), 1) % 2).astype(F32) * 0.25
    length_row = jnp.full((1, pairs), length.astype(F32))
    inv_length = 1.0 / length_row

    def turns(count, stride):
        x = (iota((count, pairs), 0) * stride).astype(F32) * waves
        return (x - jnp.floor(x * inv_length) * length_row) * inv_length

    fine = turns(8, 1) + quarter
    fine_c, fine_s = cos_turn(fine), cos_turn(fine - 0.25)
    mid = turns(16, 8)
    mid_c, mid_s = cos_turn(mid), cos_turn(mid - 0.25)
    for k in range(16):
        c, s = mid_c[k : k + 1], mid_s[k : k + 1]
        base_c[8 * k : 8 * k + 8, :] = c * fine_c - s * fine_s
        base_s[8 * k : 8 * k + 8, :] = s * fine_c + c * fine_s
    far = turns(turn_c.shape[0], LANES)
    turn_c[...] = cos_turn(far)
    turn_s[...] = cos_turn(far - 0.25)
    group = 16
    within = iota((group, pairs), 0)
    middle = -(-fields // 32) * 16
    split = [slice(0, middle), slice(middle, fields)]
    acc = [None, None]
    for n, (k, count) in enumerate(chunks):
        for g in range(0, LANES, group):
            base = base_c[g : g + group, :], base_s[g : g + group, :]
            for a in range(k, k + count):
                block = turn_c[a : a + 1, :] * base[0] - turn_s[a : a + 1, :] * base[1]
                block = jnp.where(within < length - (a * LANES + g), block, 0.0)
                t_ref[a * LANES + g : a * LANES + g + group, :] = block.astype(BF16)
        loads[n].wait()
        part = pl.ds(k * LANES, count * LANES)
        for m, some in enumerate(split):
            product = dot(gbuf[some, part], t_ref[part, :])
            acc[m] = product if n == 0 else acc[m] + product
        if n == 1:
            pl.semaphore_wait(barrier, GREETINGS)
            announce(ready)
    scale = jnp.where(2.0 * waves < length_row, inv_length, 0.0)
    for some, total in zip(split, acc):
        facc[some, :] = total * scale
    for t in range(tiles):
        s1[t] = facc[t * LANES : (t + 1) * LANES, :].T.astype(BF16)

    exchange(send1, recv1, send_sem.at[0], recv_sem.at[0], own_sem.at[0], ready)

    for copy in small[3:]:
        copy.wait()
    wave = wn_s[0, band]
    lat = lo_v[...]
    north = lat < half
    lat_row = jnp.where(north, lat, lats - 1 - lat)
    select = jnp.where(iota((half, lats), 0) == lat_row, 1.0, 0.0)
    sign = jnp.where(north, 1.0, -1.0)
    weight = dot(jnp.broadcast_to(gw_v[...], (8, half)), select, precision=HIGHEST)[0:1]
    select = select.astype(BF16)
    lat8 = jnp.broadcast_to(lat, (8, lats))
    length8 = take_lanes(jnp.broadcast_to(ll_v[...], (8, lats)), lat8)
    length_col = jnp.broadcast_to(length8[0:1].astype(F32), (lats, lats)).T
    lat_col = jnp.broadcast_to(lat.astype(F32), (lats, lats)).T
    north_col = lat_col < half
    sign_col = jnp.where(north_col, 1.0, -1.0)[:, 0:1]
    place_col = jnp.where(north_col, lat_col, lats - 1.0 - lat_col)[:, :half]
    select_t = jnp.where(iota((lats, half), 1).astype(F32) == place_col, 1.0, 0.0).astype(BF16)
    doubling = jnp.where(jnp.full((lats, lats), wave) == 0, 1.0, 2.0)
    wave_f = jnp.full((lats, lats), wave).astype(F32)
    keep_col = jnp.where(2.0 * wave_f < length_col, doubling, 0.0)[:, 0:1]

    rz[...] = jnp.zeros(rz.shape, F32)
    rz[0:1, :levels] = mr_v[...]
    rates = rz[0:1, :]
    for p in range(2):
        table = leg_v[p]
        span = slice(p * rows, (p + 1) * rows)
        degree = iota((rows, LANES), 0) * 2 + (wave + p)
        energy = (degree * (degree + 1)).astype(F32) * (STEP / float(TRUNC * (TRUNC + 1)))
        gain = weight if p == 0 else weight * sign
        own = jnp.where(degree <= TRUNC, dot(table, select, ((0,), (0,))) * gain, 0.0)
        lhs[span, :LANES] = own.astype(BF16)
        lhs[span, LANES:] = (own * -energy).astype(BF16)
        for t in range(2):
            inv[span, t * LANES : (t + 1) * LANES] = 1.0 / (
                1.0 + energy * rates[:, t * LANES : (t + 1) * LANES]
            )
        gain_col = keep_col if p == 0 else keep_col * sign_col
        l2t[:, span] = (dot(select_t, table) * gain_col).astype(BF16)
    mix = dot(l2t[...], lhs[:, :LANES]).astype(BF16)
    spread = []
    for q in range(2):
        each = jnp.where(iota((pairs, lats), 0) == iota((pairs, lats), 1) * 2 + q, 1.0, 0.0)
        each = each.astype(BF16)
        spread.append(dot(dot(each, mix).astype(BF16), each, ((1,), (1,))))
    kmix[...] = (spread[0] + spread[1]).astype(BF16)

    vz[...] = jnp.zeros(vz.shape, F32)
    cz[...] = jnp.zeros(cz.shape, F32)
    vz[:levels, :levels] = vm_v[...]
    cz[:levels, :levels] = cp_v[...]
    modes, couple = vz[...], cz[...]
    square = modes.shape
    vpad[...] = modes.astype(BF16)
    gap = levels - LANES
    shift = jnp.where(iota(square, 0) == iota(square, 1) + gap, 1.0, 0.0)
    moved = dot(shift, couple, ((1,), (1,)), precision=HIGHEST)
    gpad[...] = dot(moved, modes, precision=HIGHEST).astype(BF16)
    wide = (square[0], tiles * LANES)
    shift = jnp.where(iota(wide, 1) == iota(wide, 0) + levels, 1.0, 0.0)
    same = jnp.where(iota(wide, 1) == iota(wide, 0), 1.0, 0.0)
    spread_out = same - STEP * dot(couple, shift, ((0,), (0,)), precision=HIGHEST)
    wall[...] = dot(modes, spread_out, ((0,), (0,)), precision=HIGHEST).astype(BF16)

    wait_exchange(send1, recv1, send_sem.at[0], recv_sem.at[0], own_sem.at[0], peers)
    f0, f1, f2 = r1[0], r1[1], r1[2]
    last = jnp.concatenate([f1, f2], axis=1)
    in_d = dot(jnp.concatenate([f0, f1], axis=1), vpad[...])
    in_p = dot(last, gpad[...])
    for t in range(2):
        pf[t] = in_d[:, t * LANES : (t + 1) * LANES]
        pf[2 + t] = in_p[:, t * LANES : (t + 1) * LANES]

    parts = [pl.ds(q, lats, stride=2) for q in range(2)]
    rhs = []
    for part in parts:
        both = [jnp.concatenate([pf[n, part, :], pf[n + 1, part, :]], axis=1) for n in (0, 2)]
        rhs.append(jnp.concatenate(both, axis=0).astype(BF16))

    wide_rhs = jnp.concatenate(rhs, axis=1)
    own_p = dot(kmix[...], last)
    for k in range(0, 2 * rows, 256):
        span = slice(k, k + 256)
        each = dot(lhs[span, :], wide_rhs)
        share = inv[span, :]
        for q in range(2):
            half_q = slice(2 * q * LANES, 2 * (q + 1) * LANES)
            solved[span, half_q] = (each[:, half_q] * share).astype(BF16)
    both = dot(l2t[...], solved[...])
    totals = [both[:, : 2 * LANES], both[:, 2 * LANES :]]
    for q, part in enumerate(parts):
        for t in range(2):
            zf[t, part, :] = totals[q][:, t * LANES : (t + 1) * LANES]

    back = jnp.concatenate([zf[0], zf[1]], axis=1).astype(BF16)
    out = dot(back, wall[...])
    only_p = iota((pairs, LANES), 1) >= gap
    s2[0] = out[:, :LANES].astype(BF16)
    s2[1] = (out[:, LANES : 2 * LANES] + jnp.where(only_p, own_p[:, :LANES], 0.0)).astype(BF16)
    s2[2] = (out[:, 2 * LANES :] + own_p[:, LANES:]).astype(BF16)

    exchange(send2, recv2, send_sem.at[1], recv_sem.at[1], own_sem.at[1])
    wait_sent(send1, recv1, send_sem.at[0], peers)
    wait_exchange(send2, recv2, send_sem.at[1], recv_sem.at[1], own_sem.at[1], peers)
    for t in range(tiles):
        a_ref[t * LANES : (t + 1) * LANES, :] = r2[t].T
    wait_sent(send2, recv2, send_sem.at[1], peers)


def inverse_kernel(a_ref, t_ref, out_hbm, obuf, sem):
    fields, width = obuf.shape
    step = 4 * LANES
    copies = []
    for n, k in enumerate(range(0, width, step)):
        part = pl.ds(k, min(step, width - k))
        obuf[:, part] = dot(a_ref[:fields, :], t_ref[part, :], ((1,), (1,))).astype(BF16)
        copies.append(pltpu.make_async_copy(obuf.at[:, part], out_hbm.at[:, part], sem.at[n]))
        copies[-1].start()
    for copy in copies:
        copy.wait()


def per_device(grid_in, legendre, gauss_weight, vertical_modes, coupling, mode_rates, loop_length, lat_order, wave_number):
    fields, width = grid_in.shape[1:]
    rows, half = legendre.shape[2:]
    levels = vertical_modes.shape[0]
    lats = lat_order.shape[0]
    pairs = 2 * lats
    tiles = -(-fields // LANES)
    blocks = width // LANES
    operands = [
        grid_in.reshape(fields, width),
        jnp.swapaxes(legendre.reshape(2, rows, half), 1, 2),
        gauss_weight.reshape(1, half),
        vertical_modes,
        coupling,
        mode_rates.reshape(1, levels),
        loop_length.reshape(1, lats),
        lat_order.reshape(1, lats),
        wave_number.reshape(1, lats),
    ]
    hbm = pl.BlockSpec(memory_space=pltpu.HBM)
    vmem = pl.BlockSpec(memory_space=pltpu.VMEM)
    dma = pltpu.SemaphoreType.DMA
    a_mat, table = pl.pallas_call(
        main_kernel,
        out_shape=(
            pltpu.VMEM((tiles * LANES, pairs), BF16),
            pltpu.VMEM((width, pairs), BF16),
        ),
        in_specs=[hbm] * 9,
        out_specs=(vmem, vmem),
        scratch_shapes=[
            pltpu.VMEM((fields, width), BF16),
            pltpu.VMEM((2, half, rows), BF16),
            pltpu.VMEM((1, half), F32),
            pltpu.VMEM((levels, levels), F32),
            pltpu.VMEM((levels, levels), F32),
            pltpu.VMEM((1, levels), F32),
            pltpu.VMEM((1, lats), I32),
            pltpu.VMEM((1, lats), I32),
            pltpu.VMEM((1, lats), I32),
            pltpu.SMEM((1, lats), I32),
            pltpu.SMEM((1, lats), I32),
            pltpu.SMEM((1, lats), I32),
            pltpu.VMEM((LANES, pairs), F32),
            pltpu.VMEM((LANES, pairs), F32),
            pltpu.VMEM((-(-blocks // 8) * 8, pairs), F32),
            pltpu.VMEM((-(-blocks // 8) * 8, pairs), F32),
            pltpu.VMEM((tiles * LANES, pairs), F32),
            pltpu.VMEM((tiles, lats, 2, LANES), BF16),
            pltpu.VMEM((tiles, lats, 2, LANES), BF16),
            pltpu.VMEM((tiles, lats, 2, LANES), BF16),
            pltpu.VMEM((tiles, lats, 2, LANES), BF16),
            pltpu.VMEM((2 * rows, 2 * LANES), BF16),
            pltpu.VMEM((lats, 2 * rows), BF16),
            pltpu.VMEM((2 * rows, 2 * LANES), F32),
            pltpu.VMEM((pairs, pairs), BF16),
            pltpu.VMEM((2 * LANES, 2 * LANES), F32),
            pltpu.VMEM((2 * LANES, 2 * LANES), F32),
            pltpu.VMEM((8, 2 * LANES), F32),
            pltpu.VMEM((2 * LANES, 2 * LANES), BF16),
            pltpu.VMEM((2 * LANES, 2 * LANES), BF16),
            pltpu.VMEM((2 * LANES, tiles * LANES), BF16),
            pltpu.VMEM((4, pairs, LANES), F32),
            pltpu.VMEM((2, pairs, LANES), F32),
            pltpu.VMEM((2 * rows, 4 * LANES), BF16),
            dma((11,)),
            dma((-(-blocks // 4),)),
            dma((2,)),
            dma((2,)),
            dma((2,)),
            pltpu.SemaphoreType.REGULAR((7,)),
        ],
        compiler_params=pltpu.CompilerParams(
            collective_id=1, has_side_effects=True, vmem_limit_bytes=40 * 2**20
        ),
        name="spectral_step",
    )(*[pltpu.with_memory_space_constraint(each, pltpu.HBM) for each in operands])
    a_mat = pltpu.with_memory_space_constraint(a_mat, pltpu.VMEM)
    table = pltpu.with_memory_space_constraint(table, pltpu.VMEM)
    points = pl.pallas_call(
        inverse_kernel,
        out_shape=jax.ShapeDtypeStruct((fields, width), BF16),
        in_specs=[vmem, vmem],
        out_specs=hbm,
        scratch_shapes=[pltpu.VMEM((fields, width), BF16), dma((-(-blocks // 4),))],
        compiler_params=pltpu.CompilerParams(vmem_limit_bytes=16 * 2**20),
        name="inverse_loop",
    )(a_mat, table)
    return points.reshape(grid_in.shape)


def solution(mesh):
    whole = P(("member", "band"), None, None)
    in_specs = (whole, P("band", None, None, None)) + (P(),) * 7
    return jax.shard_map(per_device, mesh=mesh, in_specs=in_specs, out_specs=whole, check_vma=False)
```
